128 devices in a mesh: rows: 4 (over z_hi, core), cols: 32 (over x, z_lo, y).
Axes of the slice: x: 4, y: 4, z: 4 (z_hi: 2, z_lo: 2; z = z_hi * 2 + z_lo), core: 2. Of those that a mesh axis runs over, the one named last changes fastest.
Arguments:
- tokens: bfloat16 [2048, 6144], P('rows', 'cols'), may hold values from -6 to 6
- cotangent: bfloat16 [2048, 16384], P('rows', 'cols'), may hold values from -0.049804688 to 0.049804688
- weight: bfloat16 [6144, 16384], P(None, 'cols'), may hold values from -6 to 6
- momentum: float32 [128, 768, 1024], P(('rows', 'cols')), may hold values from -40 to 40
Outputs:
- new_weight: bfloat16 [6144, 16384], P(None, 'cols')
- input_grad: bfloat16 [2048, 6144], P('rows', 'cols')
- new_momentum: float32 [128, 768, 1024], P(('rows', 'cols'))
- update: float32 [128, 768, 1024], P(('rows', 'cols'))
The draws below stay inside these ranges and needn't reach their ends.
All inputs are finite; a program needn't handle non-finite values.
Results may differ from the reference program's by a relative error of at most 0.012.
Values may be sent and summed in bfloat16 or wider, within the bound.
A program may use at most 128 MiB of HBM per device.

```python
import math
import jax
import jax.numpy as jnp
from jax import lax

D = 6144
F = 16384
NS_STEPS = 2
TOKENS = 2048
BR = 768
BC = 1024
BLOCKS = 128
N_ROWS = 4
N_COLS = 32


def draw_momentum(key, part):
    key_base = jax.random.fold_in(key, 11)
    key_rows = jax.random.fold_in(key, 12)
    key_cols = jax.random.fold_in(key, 13)
    row_scale = jnp.exp(jax.random.uniform(key_rows, (BLOCKS, BR, 1), jnp.float32) * math.log(10.0))
    col_scale = jnp.exp(jax.random.uniform(key_cols, (BLOCKS, 1, BC), jnp.float32) * math.log(10.0))
    base = jnp.clip(jax.random.normal(key_base, (BLOCKS, BR, BC), jnp.float32), -4.0, 4.0)
    return (0.1 * base * row_scale * col_scale).astype(jnp.float32)


def spiked(array, stream_key, source, target, shards_of, factor):
    owner, partner = [(jnp.arange(array.shape[position]) // (array.shape[position] // shards_of)).reshape([-1 if axis == position else 1 for axis in range(array.ndim)]) for position in (source, target)]
    chosen = jax.random.permutation(stream_key, shards_of)[partner]
    strong = (owner == chosen) | (owner == (partner + shards_of // 2) % shards_of)
    return jnp.where(strong, factor * array, array)


def levels(key, shape, pieces, smallest, high):
    loudness, own = 1.0, jax.random.fold_in(key, 6)
    for axis_at, shards_of in pieces:
        draws = jnp.exp(jax.random.uniform(jax.random.fold_in(own, axis_at), (shards_of,), jnp.float32, smallest / len(pieces), high / len(pieces)))
        loudness = loudness * jnp.repeat(draws, shape[axis_at] // shards_of).reshape([-1 if axis == axis_at else 1 for axis in range(len(shape))])
    return loudness


def bell_draw(rng, shape, width, limit, pieces=(), dtype=jnp.bfloat16):
    entries = width * jax.random.normal(rng, shape, jnp.float32)
    if pieces:
        entries = entries * levels(rng, shape, pieces, -0.22, 0.18)
    return jnp.clip(entries, -limit, limit).astype(dtype)


def noise_with(key, shape, scale, reach, shards, heavy, held_as=jnp.bfloat16):
    drawn = scale * jax.random.normal(key, shape, jnp.float32)
    if shards:
        drawn = drawn * levels(key, shape, shards, -0.22, 0.18)
    return jnp.clip(spiked(drawn, jax.random.fold_in(key, 3), *heavy), -reach, reach).astype(held_as)


def setup_inputs(seed: int = 0) -> dict:
    arg_keys = jax.random.split(jax.random.key(seed), 5)
    return {
        "tokens": bell_draw(arg_keys[0], (TOKENS, D), 1.0, 6.0, ((0, 4), (1, 32))),
        "cotangent": bell_draw(arg_keys[1], (TOKENS, F), 0.0078125, 0.049804688, ((0, 4), (1, 32))),
        "weight": noise_with(arg_keys[2], (D, F), 1.0, 6.0, ((1, 32),), (1, 0, 32, 2.75)),
        "momentum": draw_momentum(jax.random.fold_in(arg_keys[4], 71), 0),
    }


coef_a = 3.4445
coef_b = -4.775
coef_c = 2.0315
beta_mom = 0.95
step_rate = 0.25

def orthogonalize(matrix):
    norm_value = jnp.sqrt(jnp.sum(matrix * matrix))
    current = (matrix / (norm_value + 1e-07)).astype(jnp.bfloat16)
    for index in range(NS_STEPS):
        square = jnp.dot(current, current.T, preferred_element_type=jnp.float32).astype(jnp.bfloat16)
        poly = (coef_b * square.astype(jnp.float32) + coef_c * jnp.dot(square, square, preferred_element_type=jnp.float32)).astype(jnp.bfloat16)
        current = (coef_a * current.astype(jnp.float32) + jnp.dot(poly, current, preferred_element_type=jnp.float32)).astype(jnp.bfloat16)
    return current

def reference(tokens, cotangent, weight, momentum):
    grad = lax.dot_general(tokens, cotangent, (((0,), (0,)), ((), ())), preferred_element_type=jnp.float32)
    input_grad = lax.dot_general(cotangent, weight, (((1,), (1,)), ((), ())), preferred_element_type=jnp.float32).astype(jnp.bfloat16)
    groups = N_ROWS
    pairs = N_COLS // 2
    blocks = grad.reshape(groups, 2, BR, pairs, BC).transpose(0, 3, 1, 2, 4).reshape(BLOCKS, BR, BC)
    new_momentum = beta_mom * momentum + blocks
    scale_value = float(max(BR, BC)) ** 0.5

    def one_block(matrix):
        return scale_value * orthogonalize(matrix).astype(jnp.float32)
    update = lax.map(one_block, new_momentum)
    placed = update.astype(jnp.bfloat16).reshape(groups, pairs, 2, BR, BC).transpose(0, 2, 3, 1, 4).reshape(D, F)
    new_weight = (weight.astype(jnp.float32) - step_rate * placed.astype(jnp.float32)).astype(jnp.bfloat16)
    return (new_weight, input_grad, new_momentum, update)
```

```python
import functools

import jax
import jax.numpy as jnp
from jax import lax
from jax.experimental import pallas as pl
from jax.experimental.pallas import tpu as pltpu
from jax.sharding import PartitionSpec as P

NS_STEPS = 2
TOK = 512
FEAT = 192
BR = 768
BC = 1024
HALF = 512
COEF_A = 3.4445
COEF_B = -4.775
COEF_C = 2.0315
BETA = 0.95

MESH = pl.DeviceIdType.MESH
F32 = jnp.float32
BF16 = jnp.bfloat16


def place():
    r = lax.axis_index("rows")
    c = lax.axis_index("cols")
    return r, c, c // 8, (c // 4) % 2, c % 4


def remote(src, dst, send, recv, r, c):
    return pltpu.make_async_remote_copy(
        src_ref=src,
        dst_ref=dst,
        send_sem=send,
        recv_sem=recv,
        device_id=(r, c),
        device_id_type=MESH,
    )


def spread_targets():
    r, c, x, zl, y = place()
    out = []
    for zd in range(2):
        for yb in range(2):
            col = r * 8 + zd * 4 + zl + 2 * yb
            out.append((x, col, (x == r) & (col == c)))
    return out


def spread_sources():
    r, c, x, zl, y = place()
    return [(x, r * 8 + (y % 2) * 4 + k, (x == r) & (r * 8 + (y % 2) * 4 + k == c)) for k in range(4)]


def x_neighbours():
    r, c, x, zl, y = place()
    low = c % 8
    return ((x + 3) % 4) * 8 + low, ((x + 1) % 4) * 8 + low


def signal_unless(flag, barrier, r, c):
    @pl.when(jnp.logical_not(flag))
    def _():
        pl.semaphore_signal(barrier, inc=1, device_id=(r, c), device_id_type=MESH)


def entry_barrier():
    r, c, x, zl, y = place()
    left, right = x_neighbours()
    barrier = pltpu.get_barrier_semaphore()
    for rd, cd in ((r, left), (r, right), (r ^ 2, c), (r, c ^ 1), (r ^ 2, c ^ 1), (r ^ 1, c)):
        pl.semaphore_signal(barrier, inc=1, device_id=(rd, cd), device_id_type=MESH)
    targets, sources = spread_targets(), spread_sources()
    for rd, cd, own in targets + sources:
        signal_unless(own, barrier, rd, cd)
    own_count = sum(jnp.where(own, 1, 0) for _, _, own in targets + sources)
    pl.semaphore_wait(barrier, 14 - own_count)


def gather_kernel(
    tok_ref, cot_ref, w_ref, grad_ref, terms_ref,
    tokg, cotg, wcat, gacc, tbuf,
    s1s, s1r, xs, xr, cs, cr, ds_, dr, ws, wr, ls, os_,
):
    r, c, x, zl, y = place()
    h = c % 2
    o = 1 - h
    left, right = x_neighbours()
    entry_barrier()

    def rows_of(group):
        return pl.ds(pl.multiple_of(group * TOK, TOK), TOK)

    def half_of(which):
        return pl.ds(pl.multiple_of(which * HALF, HALF), HALF)

    sends = []
    for k, (rd, cd, own) in enumerate(spread_targets()):
        dst = tokg.at[pl.ds(pl.multiple_of(y * FEAT, FEAT), FEAT), rows_of(r)]
        cp = remote(tok_ref, dst, s1s.at[k], s1r.at[y], rd, cd)
        here = pltpu.make_async_copy(tok_ref, dst, s1r.at[y])

        @pl.when(jnp.logical_not(own))
        def _():
            cp.start()

        @pl.when(own)
        def _():
            here.start()

        sends.append((cp, own))

    mine = cotg.at[rows_of(r), half_of(h)]
    peers = ((r, c ^ 1), (r ^ 2, c), (r ^ 2, c ^ 1))
    direct = []
    for k, (rd, cd) in enumerate(peers):
        cp = remote(cot_ref, mine, cs.at[k], cr.at[k], rd, cd)
        cp.start()
        direct.append(cp)
    core = [remote(cot_ref, mine, ds_.at[3], dr.at[3], r ^ 1, c)]
    core[0].start()
    own_cot = pltpu.make_async_copy(cot_ref, mine, ls.at[0])
    own_cot.start()

    wsend = remote(
        w_ref.at[pl.ds(pl.multiple_of((2 * r + o) * BR, BR), BR), :],
        wcat.at[:, half_of(h)], ws.at[0], wr.at[0], r, c ^ 1,
    )
    wsend.start()
    own_w = pltpu.make_async_copy(
        w_ref.at[pl.ds(pl.multiple_of((2 * r + h) * BR, BR), BR), :], wcat.at[:, half_of(h)], ls.at[1]
    )
    own_w.start()

    ring = []
    for k in range(4):
        piece = tokg.at[pl.ds(k * FEAT, FEAT), rows_of(x)]
        pltpu.make_async_copy(piece, piece, s1r.at[k]).wait()
        for d, cd in ((0, left), (1, right)):
            cp = remote(piece, piece, xs.at[d, k], xr.at[d, k], r, cd)
            cp.start()
            ring.append(cp)

    froms = ((r, o), (r ^ 2, h), (r ^ 2, o))
    for k, (rs, hs) in enumerate(froms):
        ref = cotg.at[rows_of(rs), half_of(hs)]
        pltpu.make_async_copy(ref, ref, cr.at[k]).wait()
        cp = remote(ref, ref, ds_.at[k], dr.at[k], r ^ 1, c)
        cp.start()
        core.append(cp)

    xl, xr_ = (x + 3) % 4, (x + 1) % 4
    for k in range(2):
        ref = tokg.at[pl.ds(k * FEAT, FEAT), rows_of(xl)]
        pltpu.make_async_copy(ref, ref, xr.at[1, k]).wait()
        cp = remote(ref, ref, xs.at[2, k], xr.at[2, k], r, right)
        cp.start()
        ring.append(cp)
        ref = tokg.at[pl.ds((k + 2) * FEAT, FEAT), rows_of(xr_)]
        pltpu.make_async_copy(ref, ref, xr.at[0, k + 2]).wait()
        cp = remote(ref, ref, xs.at[2, k + 2], xr.at[2, k + 2], r, left)
        cp.start()
        ring.append(cp)

    own_cot.wait()
    for k, (rs, hs) in enumerate(((r ^ 1, o), (r ^ 3, h), (r ^ 3, o), (r ^ 1, h))):
        ref = cotg.at[rows_of(rs), half_of(hs)]
        pltpu.make_async_copy(ref, ref, dr.at[k]).wait()

    def grad_step(group, first):
        def tile(i, carry):
            rows = pl.ds(pl.multiple_of(i * 256, 256), 256)
            part = jnp.dot(tokg[rows, rows_of(group)], cotg[rows_of(group), :], preferred_element_type=F32)
            gacc[rows, :] = part if first else gacc[rows, :] + part
            return carry

        lax.fori_loop(0, BR // 256, tile, 0)

    grad_step(x, True)
    for k in range(2):
        ref = tokg.at[pl.ds(k * FEAT, FEAT), rows_of(xr_)]
        pltpu.make_async_copy(ref, ref, xr.at[0, k]).wait()
        ref = tokg.at[pl.ds((k + 2) * FEAT, FEAT), rows_of(xl)]
        pltpu.make_async_copy(ref, ref, xr.at[1, k + 2]).wait()
    grad_step(xl, False)
    grad_step(xr_, False)

    own_w.wait()
    pltpu.make_async_copy(wcat.at[:, half_of(o)], wcat.at[:, half_of(o)], wr.at[0]).wait()

    def terms_step(group, carry):
        def tile(i, inner):
            rows = pl.ds(pl.multiple_of(i * 256, 256), 256)
            part = lax.dot_general(
                wcat[rows, :], cotg[rows_of(group), :], (((1,), (1,)), ((), ())), preferred_element_type=F32
            )
            tbuf[rows, rows_of(group)] = part.astype(BF16)
            return inner

        return lax.fori_loop(0, BR // 256, tile, carry)

    lax.fori_loop(0, 4, terms_step, 0)
    out_terms = pltpu.make_async_copy(tbuf, terms_ref, os_.at[0])
    out_terms.start()

    x2 = (x + 2) % 4
    for k in range(4):
        ref = tokg.at[pl.ds(k * FEAT, FEAT), rows_of(x2)]
        pltpu.make_async_copy(ref, ref, xr.at[2, k]).wait()
    grad_step(x2, False)
    out_grad = pltpu.make_async_copy(gacc, grad_ref, os_.at[1])
    out_grad.start()

    for cp, own in sends:
        @pl.when(jnp.logical_not(own))
        def _():
            cp.wait_send()
    for cp in ring + direct + core + [wsend]:
        cp.wait_send()
    out_terms.wait()
    out_grad.wait()


def gather_call(tok, cot, weight):
    any_ = pl.BlockSpec(memory_space=pl.ANY)
    dma = pltpu.SemaphoreType.DMA
    return pl.pallas_call(
        gather_kernel,
        out_shape=(
            jax.ShapeDtypeStruct((BR, BC), F32),
            jax.ShapeDtypeStruct((BR, 4 * TOK), BF16),
        ),
        in_specs=[any_, any_, any_],
        out_specs=(any_, any_),
        scratch_shapes=[
            pltpu.VMEM((BR, 4 * TOK), BF16),
            pltpu.VMEM((4 * TOK, BC), BF16),
            pltpu.VMEM((BR, BC), BF16),
            pltpu.VMEM((BR, BC), F32),
            pltpu.VMEM((BR, 4 * TOK), BF16),
            dma((4,)), dma((4,)), dma((3, 4)), dma((3, 4)), dma((3,)), dma((3,)),
            dma((4,)), dma((4,)), dma((1,)), dma((1,)), dma((2,)), dma((2,)),
        ],
        compiler_params=pltpu.CompilerParams(
            collective_id=0, has_side_effects=True, vmem_limit_bytes=48 << 20
        ),
        cost_estimate=pl.CostEstimate(flops=7_000_000_000, bytes_accessed=20_000_000, transcendentals=0),
        name="gather_dots",
    )(tok, cot, weight)


def tiles(step, rows=256):
    def run(i, carry):
        step(pl.ds(pl.multiple_of(i * rows, rows), rows))
        return carry

    lax.fori_loop(0, BR // rows, run, 0)


def ortho_kernel(grad_ref, mom_ref, newm_ref, upd_ref, x_ref, sq, ab, xb):
    sq[...] = jnp.zeros_like(sq)

    def momentum(rows):
        new = BETA * mom_ref[rows, :] + grad_ref[rows, :]
        newm_ref[rows, :] = new
        sq[...] += jnp.sum((new * new).reshape(-1, 8, BC), axis=0)

    tiles(momentum, 64)
    norm = jnp.sqrt(jnp.sum(sq[...])) + 1e-07

    def first(rows):
        x_ref[rows, :] = (newm_ref[rows, :] / norm).astype(BF16)

    tiles(first, 64)
    nt = (((1,), (1,)), ((), ()))
    src, dst = x_ref, xb
    for step in range(NS_STEPS):
        def gram(rows):
            ab[0, rows, :] = lax.dot_general(src[rows, :], src[...], nt, preferred_element_type=F32).astype(BF16)

        def poly(rows):
            a = ab[0, rows, :]
            aa = jnp.dot(a, ab[0], preferred_element_type=F32)
            ab[1, rows, :] = (COEF_B * a.astype(F32) + COEF_C * aa).astype(BF16)

        last = step == NS_STEPS - 1

        def apply(rows):
            bx = jnp.dot(ab[1, rows, :], src[...], preferred_element_type=F32)
            new = (COEF_A * src[rows, :].astype(F32) + bx).astype(BF16)
            dst[rows, :] = new
            if last:
                upd_ref[rows, :] = 32.0 * new.astype(F32)

        tiles(gram)
        tiles(poly)
        tiles(apply)
        src, dst = dst, src


def ortho_call(grad, momentum):
    vm = pl.BlockSpec(memory_space=pltpu.VMEM)
    return pl.pallas_call(
        ortho_kernel,
        out_shape=(
            jax.ShapeDtypeStruct((BR, BC), F32),
            jax.ShapeDtypeStruct((BR, BC), F32),
            jax.ShapeDtypeStruct((BR, BC), BF16),
        ),
        in_specs=[vm, vm],
        out_specs=(vm, vm, vm),
        scratch_shapes=[
            pltpu.VMEM((8, BC), F32),
            pltpu.VMEM((2, BR, BR), BF16),
            pltpu.VMEM((BR, BC), BF16),
        ],
        compiler_params=pltpu.CompilerParams(vmem_limit_bytes=40 << 20),
        cost_estimate=pl.CostEstimate(flops=7_000_000_000, bytes_accessed=14_000_000, transcendentals=0),
        name="momentum_ortho",
    )(grad, momentum)


def scatter_kernel(
    terms_ref, x_ref, w_ref, ig_ref, neww_ref,
    tb, fl, fr, sb, ib, igb, ub, wb,
    xs, xr, cs, cr, ds_, dr, s2s, s2r, ls, os_,
):
    r, c, x, zl, y = place()
    h = c % 2
    o = 1 - h
    left, right = x_neighbours()
    load_w = pltpu.make_async_copy(w_ref, wb, ls.at[0])
    load_w.start()
    load_t = pltpu.make_async_copy(terms_ref, tb, ls.at[1])
    load_t.start()
    entry_barrier()

    def rows_of(group):
        return pl.ds(pl.multiple_of(group * TOK, TOK), TOK)

    def half_of(which):
        return pl.ds(pl.multiple_of(which * HALF, HALF), HALF)

    xl, xr_, x2 = (x + 3) % 4, (x + 1) % 4, (x + 2) % 4
    MID = BR // 2
    top, low = pl.ds(0, MID), pl.ds(MID, MID)

    own_x = x_ref.at[:, half_of(h)]
    other_x = x_ref.at[:, half_of(o)]
    slot = ub.at[2 * r + h]
    direct = []
    for k, (src, rd, cd) in enumerate(((other_x, r, c ^ 1), (own_x, r ^ 2, c), (other_x, r ^ 2, c ^ 1))):
        cp = remote(src, slot, cs.at[k], cr.at[k], rd, cd)
        cp.start()
        direct.append(cp)
    core = [remote(own_x, slot, ds_.at[3], dr.at[3], r ^ 1, c)]
    core[0].start()
    own_u = pltpu.make_async_copy(own_x, slot, ls.at[2])
    own_u.start()

    ring = []

    def send(src, dst, i, j, cd):
        cp = remote(src, dst, xs.at[i, j], xr.at[i, j], r, cd)
        cp.start()
        ring.append(cp)

    load_t.wait()
    send(tb.at[top, rows_of(x2)], fl.at[0], 0, 0, right)
    send(tb.at[low, rows_of(x2)], fr.at[0], 1, 0, left)
    send(tb.at[low, rows_of(xr_)], fl.at[2], 0, 1, right)
    send(tb.at[top, rows_of(xl)], fr.at[2], 1, 1, left)
    pltpu.make_async_copy(fl.at[0], fl.at[0], xr.at[0, 0]).wait()

    def join(src, rows, group):
        def step(i, carry):
            part = pl.ds(pl.multiple_of(i * 64, 64), 64)
            here = pl.ds(pl.multiple_of(rows + i * 64, 64), 64)
            src[0, part, :] = (
                src[0, part, :].astype(F32) + tb[here, rows_of(group)].astype(F32)
            ).astype(BF16)
            return carry

        lax.fori_loop(0, MID // 64, step, 0)

    join(fl, 0, xr_)
    send(fl.at[0], fl.at[1], 0, 2, right)
    pltpu.make_async_copy(fr.at[0], fr.at[0], xr.at[1, 0]).wait()
    join(fr, MID, xl)
    send(fr.at[0], fr.at[1], 1, 2, left)

    def update_rows(rs, hs):
        at = 2 * rs + hs

        def step(i, carry):
            part = pl.ds(pl.multiple_of(i * 64, 64), 64)
            here = pl.ds(pl.multiple_of(at * BR + i * 64, 64), 64)
            wb[here, :] = (wb[here, :].astype(F32) - 8.0 * ub[at, part, :].astype(F32)).astype(BF16)
            return carry

        lax.fori_loop(0, BR // 64, step, 0)
        rows = pl.ds(pl.multiple_of(at * BR, BR), BR)
        cp = pltpu.make_async_copy(wb.at[rows, :], neww_ref.at[rows, :], os_.at[at])
        cp.start()
        return cp

    outs = []
    load_w.wait()
    own_u.wait()
    outs.append(update_rows(r, h))
    pltpu.make_async_copy(slot, slot, dr.at[3]).wait()
    outs.append(update_rows(r ^ 1, h))

    for ref, i, j in ((fl, 0, 1), (fr, 1, 1), (fl, 0, 2), (fr, 1, 2)):
        at = 2 if j == 1 else 1
        pltpu.make_async_copy(ref.at[at], ref.at[at], xr.at[i, j]).wait()

    def total(i, carry):
        part = pl.ds(pl.multiple_of(i * 64, 64), 64)
        below = pl.ds(pl.multiple_of(MID + i * 64, 64), 64)
        sb[part, :] = (
            tb[part, rows_of(x)].astype(F32) + fl[1, part, :].astype(F32) + fr[2, part, :].astype(F32)
        ).astype(BF16)
        sb[below, :] = (
            tb[below, rows_of(x)].astype(F32) + fr[1, part, :].astype(F32) + fl[2, part, :].astype(F32)
        ).astype(BF16)
        return carry

    lax.fori_loop(0, MID // 64, total, 0)
    last = []
    for k, (rd, cd, own) in enumerate(spread_sources()):
        piece = sb.at[pl.ds(k * FEAT, FEAT), :]
        at = zl * 2 + y // 2
        cp = remote(piece, ib.at[at], s2s.at[k], s2r.at[at], rd, cd)
        here = pltpu.make_async_copy(piece, ib.at[at], s2r.at[at])

        @pl.when(jnp.logical_not(own))
        def _():
            cp.start()

        @pl.when(own)
        def _():
            here.start()

        last.append((cp, own))

    froms = ((r, o), (r ^ 2, h), (r ^ 2, o))
    for k, (rs, hs) in enumerate(froms):
        ref = ub.at[2 * rs + hs]
        pltpu.make_async_copy(ref, ref, cr.at[k]).wait()
        cp = remote(ref, ref, ds_.at[k], dr.at[k], r ^ 1, c)
        cp.start()
        core.append(cp)
        outs.append(update_rows(rs, hs))

    for k in range(4):
        pltpu.make_async_copy(ib.at[k], ib.at[k], s2r.at[k]).wait()
    igb[...] = (
        (ib[0].astype(F32) + ib[1].astype(F32)) + (ib[2].astype(F32) + ib[3].astype(F32))
    ).astype(BF16)
    out_ig = pltpu.make_async_copy(igb, ig_ref, os_.at[8])
    out_ig.start()

    for k, (rs, hs) in enumerate(((r ^ 1, o), (r ^ 3, h), (r ^ 3, o))):
        ref = ub.at[2 * rs + hs]
        pltpu.make_async_copy(ref, ref, dr.at[k]).wait()
        outs.append(update_rows(rs, hs))

    for cp, own in last:
        @pl.when(jnp.logical_not(own))
        def _():
            cp.wait_send()
    for cp in ring + direct + core:
        cp.wait_send()
    for cp in outs:
        cp.wait()
    out_ig.wait()


def scatter_call(terms, xmat, weight):
    any_ = pl.BlockSpec(memory_space=pl.ANY)
    dma = pltpu.SemaphoreType.DMA
    return pl.pallas_call(
        scatter_kernel,
        out_shape=(
            jax.ShapeDtypeStruct((FEAT, TOK), BF16),
            jax.ShapeDtypeStruct(weight.shape, BF16),
        ),
        in_specs=[any_, pl.BlockSpec(memory_space=pltpu.VMEM), any_],
        out_specs=(any_, any_),
        scratch_shapes=[
            pltpu.VMEM((BR, 4 * TOK), BF16),
            pltpu.VMEM((3, BR // 2, TOK), BF16),
            pltpu.VMEM((3, BR // 2, TOK), BF16),
            pltpu.VMEM((BR, TOK), BF16),
            pltpu.VMEM((4, FEAT, TOK), BF16),
            pltpu.VMEM((FEAT, TOK), BF16),
            pltpu.VMEM((8, BR, HALF), BF16),
            pltpu.VMEM(weight.shape, BF16),
            dma((2, 3)), dma((2, 3)), dma((3,)), dma((3,)), dma((4,)), dma((4,)),
            dma((4,)), dma((4,)), dma((3,)), dma((9,)),
        ],
        compiler_params=pltpu.CompilerParams(
            collective_id=1, has_side_effects=True, vmem_limit_bytes=48 << 20
        ),
        cost_estimate=pl.CostEstimate(flops=20_000_000, bytes_accessed=20_000_000, transcendentals=0),
        name="scatter_update",
    )(terms, xmat, weight)


def body(tokens, cotangent, weight, momentum):
    grad, terms = gather_call(tokens.T, cotangent, weight)
    new_momentum, update, xmat = ortho_call(grad, momentum[0])
    input_grad, new_weight = scatter_call(terms, xmat, weight)
    return new_weight, input_grad.T, new_momentum[None], update[None]


def solution(mesh):
    in_specs = (P("rows", "cols"), P("rows", "cols"), P(None, "cols"), P(("rows", "cols"), None, None))
    out_specs = (
        P(None, "cols"),
        P("rows", "cols"),
        P(("rows", "cols"), None, None),
        P(("rows", "cols"), None, None),
    )
    return jax.shard_map(body, mesh=mesh, in_specs=in_specs, out_specs=out_specs, check_vma=False)
```

```python
import functools

import jax
import jax.numpy as jnp
from jax import lax
from jax.experimental import pallas as pl
from jax.experimental.pallas import tpu as pltpu
from jax.sharding import PartitionSpec as P

NS_STEPS = 2
TOK = 512
FEAT = 192
BR = 768
BC = 1024
HALF = 512
COEF_A = 3.4445
COEF_B = -4.775
COEF_C = 2.0315
BETA = 0.95

MESH = pl.DeviceIdType.MESH
F32 = jnp.float32
BF16 = jnp.bfloat16


def place():
    r = lax.axis_index("rows")
    c = lax.axis_index("cols")
    return r, c, c // 8, (c // 4) % 2, c % 4


def remote(src, dst, send, recv, r, c):
    return pltpu.make_async_remote_copy(
        src_ref=src,
        dst_ref=dst,
        send_sem=send,
        recv_sem=recv,
        device_id=(r, c),
        device_id_type=MESH,
    )


def flip(v):
    return (v % 2) * 2 + v // 2


def group_at(x, r):
    return flip((x + 4 - r) % 4)


def spread_targets():
    r, c, x, zl, y = place()
    out = []
    for zd in range(2):
        for yb in range(2):
            col = ((x + flip(r)) % 4) * 8 + zd * 4 + zl + 2 * yb
            out.append((x, col, (x == r) & (col == c)))
    return out


def spread_sources():
    r, c, x, zl, y = place()
    group = group_at(x, r)
    base = r * 8 + (y % 2) * 4
    return [(group, base + k, (group == r) & (base + k == c)) for k in range(4)]


def x_neighbours():
    r, c, x, zl, y = place()
    low = c % 8
    return ((x + 3) % 4) * 8 + low, ((x + 1) % 4) * 8 + low


def signal_unless(flag, barrier, r, c):
    @pl.when(jnp.logical_not(flag))
    def _():
        pl.semaphore_signal(barrier, inc=1, device_id=(r, c), device_id_type=MESH)


def entry_barrier():
    r, c, x, zl, y = place()
    left, right = x_neighbours()
    barrier = pltpu.get_barrier_semaphore()
    for rd, cd in ((r, left), (r, right), (r ^ 2, c), (r, c ^ 1), (r ^ 1, c)):
        pl.semaphore_signal(barrier, inc=1, device_id=(rd, cd), device_id_type=MESH)
    targets, sources = spread_targets(), spread_sources()
    for rd, cd, own in targets + sources:
        signal_unless(own, barrier, rd, cd)
    own_count = sum(jnp.where(own, 1, 0) for _, _, own in targets + sources)
    pl.semaphore_wait(barrier, 13 - own_count)


def rows_of(group):
    return pl.ds(pl.multiple_of(group * TOK, TOK), TOK)


def half_of(which):
    return pl.ds(pl.multiple_of(which * HALF, HALF), HALF)


def arrived(ref, sem):
    pltpu.make_async_copy(ref, ref, sem).wait()


def tiles(step, rows=256):
    def run(i, carry):
        step(pl.ds(pl.multiple_of(i * rows, rows), rows))
        return carry

    lax.fori_loop(0, BR // rows, run, 0)


def gather_kernel(
    tok_ref, cot_ref, w_ref, grad_ref, terms_ref,
    tokv, tokg, cotg, wcat, gacc, tacc,
    s1s, s1r, xs, xr, cs, cr, ds_, dr, ws, wr, ls,
):
    r, c, x, zl, y = place()
    h = c % 2
    o = 1 - h
    left, right = x_neighbours()
    mine = cotg.at[rows_of(r), half_of(h)]
    own_tok = pltpu.make_async_copy(tok_ref, tokv, ls.at[0])
    own_cot = pltpu.make_async_copy(cot_ref, mine, ls.at[1])
    own_w = pltpu.make_async_copy(
        w_ref.at[pl.ds(pl.multiple_of((2 * r + h) * BR, BR), BR), :], wcat.at[:, half_of(h)], ls.at[2]
    )
    own_tok.start()
    own_cot.start()
    own_w.start()
    entry_barrier()
    own_tok.wait()

    sends = []
    for k, (rd, cd, own) in enumerate(spread_targets()):
        dst = tokg.at[pl.ds(pl.multiple_of(y * FEAT, FEAT), FEAT), rows_of(r)]
        cp = remote(tokv, dst, s1s.at[k], s1r.at[y], rd, cd)
        here = pltpu.make_async_copy(tokv, dst, s1r.at[y])

        @pl.when(jnp.logical_not(own))
        def _():
            cp.start()

        @pl.when(own)
        def _():
            here.start()

        sends.append((cp, own))

    own_cot.wait()
    others = []

    def send(src, dst, ss, rs, rd, cd):
        cp = remote(src, dst, ss, rs, rd, cd)
        cp.start()
        others.append(cp)

    send(mine, mine, cs.at[0], cr.at[0], r, c ^ 1)
    send(mine, mine, cs.at[1], cr.at[1], r ^ 2, c)
    send(mine, mine, ds_.at[3], dr.at[3], r ^ 1, c)

    send(
        w_ref.at[pl.ds(pl.multiple_of((2 * r + o) * BR, BR), BR), :],
        wcat.at[:, half_of(h)], ws.at[0], wr.at[0], r, c ^ 1,
    )

    q0, ql, qr, q2 = (group_at((x + k) % 4, r) for k in (0, 3, 1, 2))
    for k in range(4):
        piece = tokg.at[pl.ds(k * FEAT, FEAT), rows_of(q0)]
        arrived(piece, s1r.at[k])
        send(piece, piece, xs.at[0, k], xr.at[0, k], r, left)
        send(piece, piece, xs.at[1, k], xr.at[1, k], r, right)

    froms = ((r, o), (r ^ 2, h), (r ^ 2, o))

    def pass_on(k):
        ref = cotg.at[rows_of(froms[k][0]), half_of(froms[k][1])]
        arrived(ref, cr.at[k])
        if k == 0:
            send(ref, ref, cs.at[2], cr.at[2], r ^ 2, c)
        send(ref, ref, ds_.at[k], dr.at[k], r ^ 1, c)

    pass_on(0)
    pass_on(1)

    for k in range(2):
        ref = tokg.at[pl.ds(k * FEAT, FEAT), rows_of(ql)]
        arrived(ref, xr.at[1, k])
        send(ref, ref, xs.at[2, k], xr.at[2, k], r, right)
        ref = tokg.at[pl.ds((k + 2) * FEAT, FEAT), rows_of(qr)]
        arrived(ref, xr.at[0, k + 2])
        send(ref, ref, xs.at[2, k + 2], xr.at[2, k + 2], r, left)

    def from_core(k, rs, hs):
        arrived(cotg.at[rows_of(rs), half_of(hs)], dr.at[k])

    own_w.wait()
    from_core(3, r ^ 1, h)
    from_core(1, r ^ 3, h)
    nt = (((1,), (1,)), ((), ()))

    def terms_half(which, first):
        def step(group, carry):
            def tile(rows):
                part = lax.dot_general(
                    wcat[rows, half_of(which)], cotg[rows_of(group), half_of(which)], nt,
                    preferred_element_type=F32,
                )
                if first:
                    tacc[rows, rows_of(group)] = part
                else:
                    terms_ref[rows, rows_of(group)] = (tacc[rows, rows_of(group)] + part).astype(BF16)

            tiles(tile)
            return carry

        lax.fori_loop(0, 4, step, 0)

    terms_half(h, True)
    pass_on(2)
    from_core(0, r ^ 1, o)
    from_core(2, r ^ 3, o)

    def grad_step(group, first, last=False):
        def tile(rows):
            part = jnp.dot(tokg[rows, rows_of(group)], cotg[rows_of(group), :], preferred_element_type=F32)
            total = part if first else gacc[rows, :] + part
            if last:
                grad_ref[rows, :] = total
            else:
                gacc[rows, :] = total

        tiles(tile)

    grad_step(q0, True)
    for k in range(2):
        arrived(tokg.at[pl.ds(k * FEAT, FEAT), rows_of(qr)], xr.at[0, k])
        arrived(tokg.at[pl.ds((k + 2) * FEAT, FEAT), rows_of(ql)], xr.at[1, k + 2])
    grad_step(ql, False)
    grad_step(qr, False)
    arrived(wcat.at[:, half_of(o)], wr.at[0])
    terms_half(o, False)
    for k in range(4):
        arrived(tokg.at[pl.ds(k * FEAT, FEAT), rows_of(q2)], xr.at[2, k])
    grad_step(q2, False, True)

    for cp, own in sends:
        @pl.when(jnp.logical_not(own))
        def _():
            cp.wait_send()
    for cp in others:
        cp.wait_send()


def gather_call(tok, cot, weight):
    hbm = pl.BlockSpec(memory_space=pltpu.HBM)
    vm = pl.BlockSpec(memory_space=pltpu.VMEM)
    dma = pltpu.SemaphoreType.DMA
    return pl.pallas_call(
        gather_kernel,
        out_shape=(
            jax.ShapeDtypeStruct((BR, BC), F32),
            jax.ShapeDtypeStruct((BR, 4 * TOK), BF16),
        ),
        in_specs=[hbm, hbm, hbm],
        out_specs=(vm, vm),
        scratch_shapes=[
            pltpu.VMEM((FEAT, TOK), BF16),
            pltpu.VMEM((BR, 4 * TOK), BF16),
            pltpu.VMEM((4 * TOK, BC), BF16),
            pltpu.VMEM((BR, BC), BF16),
            pltpu.VMEM((BR, BC), F32),
            pltpu.VMEM((BR, 4 * TOK), F32),
            dma((4,)), dma((4,)), dma((3, 4)), dma((3, 4)), dma((3,)), dma((3,)),
            dma((4,)), dma((4,)), dma((1,)), dma((1,)), dma((3,)),
        ],
        compiler_params=pltpu.CompilerParams(
            collective_id=0, has_side_effects=True, vmem_limit_bytes=48_000_000
        ),
        cost_estimate=pl.CostEstimate(flops=7_000_000_000, bytes_accessed=20_000_000, transcendentals=0),
        name="gather_dots",
    )(tok, cot, weight)


def ortho_scatter_kernel(
    grad_ref, mom_ref, terms_ref, w_ref, newm_ref, x_ref, ig_ref, neww_ref,
    sq, ab, xb, fl, fr, sb, ib, ub,
    xs, xr, cs, cr, ds_, dr, s2s, s2r, ls,
):
    r, c, x, zl, y = place()
    h = c % 2
    o = 1 - h
    left, right = x_neighbours()
    load_w = pltpu.make_async_copy(w_ref, neww_ref, ls.at[0])
    load_w.start()
    entry_barrier()
    q0, ql, qr, q2 = (group_at((x + k) % 4, r) for k in (0, 3, 1, 2))
    MID = BR // 2
    top, low = pl.ds(0, MID), pl.ds(MID, MID)
    others = []

    def send(src, dst, ss, rs, rd, cd):
        cp = remote(src, dst, ss, rs, rd, cd)
        cp.start()
        others.append(cp)

    send(terms_ref.at[top, rows_of(q2)], fl.at[0], xs.at[0, 0], xr.at[0, 0], r, right)
    send(terms_ref.at[low, rows_of(q2)], fr.at[0], xs.at[1, 0], xr.at[1, 0], r, left)
    send(terms_ref.at[low, rows_of(qr)], fl.at[2], xs.at[0, 1], xr.at[0, 1], r, right)
    send(terms_ref.at[top, rows_of(ql)], fr.at[2], xs.at[1, 1], xr.at[1, 1], r, left)

    def join(src, base, group):
        def step(i, carry):
            part = pl.ds(pl.multiple_of(i * 64, 64), 64)
            here = pl.ds(pl.multiple_of(base + i * 64, 64), 64)
            src[0, part, :] = (
                src[0, part, :].astype(F32) + terms_ref[here, rows_of(group)].astype(F32)
            ).astype(BF16)
            return carry

        lax.fori_loop(0, MID // 64, step, 0)

    sq[...] = jnp.zeros_like(sq)

    def momentum(rows):
        new = BETA * mom_ref[rows, :] + grad_ref[rows, :]
        newm_ref[rows, :] = new
        sq[...] += jnp.sum((new * new).reshape(-1, 8, BC), axis=0)

    tiles(momentum, 64)
    norm = jnp.sqrt(jnp.sum(sq[...])) + 1e-07

    def first(rows):
        x_ref[rows, :] = (newm_ref[rows, :] / norm).astype(BF16)

    tiles(first, 64)
    nt = (((1,), (1,)), ((), ()))
    src, dst = x_ref, xb
    for step in range(NS_STEPS):
        def gram(rows):
            ab[0, rows, :] = lax.dot_general(src[rows, :], src[...], nt, preferred_element_type=F32).astype(BF16)

        def poly(rows):
            a = ab[0, rows, :]
            aa = jnp.dot(a, ab[0], preferred_element_type=F32)
            ab[1, rows, :] = (COEF_B * a.astype(F32) + COEF_C * aa).astype(BF16)

        def apply(rows):
            bx = jnp.dot(ab[1, rows, :], src[...], preferred_element_type=F32)
            dst[rows, :] = (COEF_A * src[rows, :].astype(F32) + bx).astype(BF16)

        tiles(gram)
        tiles(poly)
        tiles(apply)
        if step == 0:
            arrived(fl.at[0], xr.at[0, 0])
            join(fl, 0, qr)
            send(fl.at[0], fl.at[1], xs.at[0, 2], xr.at[0, 2], r, right)
            arrived(fr.at[0], xr.at[1, 0])
            join(fr, MID, ql)
            send(fr.at[0], fr.at[1], xs.at[1, 2], xr.at[1, 2], r, left)
        src, dst = dst, src

    own_x = x_ref.at[:, half_of(h)]
    other_x = x_ref.at[:, half_of(o)]
    slot = ub.at[2 * r + h]
    send(other_x, slot, cs.at[0], cr.at[0], r, c ^ 1)
    send(own_x, slot, cs.at[1], cr.at[1], r ^ 2, c)
    send(own_x, slot, ds_.at[3], dr.at[3], r ^ 1, c)
    own_u = pltpu.make_async_copy(own_x, slot, ls.at[1])
    own_u.start()

    def update_rows(rs, hs):
        at = 2 * rs + hs

        def step(i, carry):
            part = pl.ds(pl.multiple_of(i * 64, 64), 64)
            here = pl.ds(pl.multiple_of(at * BR + i * 64, 64), 64)
            neww_ref[here, :] = (neww_ref[here, :].astype(F32) - 8.0 * ub[at, part, :].astype(F32)).astype(BF16)
            return carry

        lax.fori_loop(0, BR // 64, step, 0)

    load_w.wait()
    own_u.wait()
    update_rows(r, h)
    arrived(slot, dr.at[3])
    update_rows(r ^ 1, h)

    for ref, i, j in ((fl, 0, 1), (fr, 1, 1), (fl, 0, 2), (fr, 1, 2)):
        arrived(ref.at[3 - j], xr.at[i, j])

    def total(i, carry):
        part = pl.ds(pl.multiple_of(i * 64, 64), 64)
        below = pl.ds(pl.multiple_of(MID + i * 64, 64), 64)
        sb[part, :] = (
            terms_ref[part, rows_of(q0)].astype(F32) + fl[1, part, :].astype(F32) + fr[2, part, :].astype(F32)
        ).astype(BF16)
        sb[below, :] = (
            terms_ref[below, rows_of(q0)].astype(F32) + fr[1, part, :].astype(F32) + fl[2, part, :].astype(F32)
        ).astype(BF16)
        return carry

    lax.fori_loop(0, MID // 64, total, 0)
    last = []
    for k, (rd, cd, own) in enumerate(spread_sources()):
        piece = sb.at[pl.ds(k * FEAT, FEAT), :]
        at = zl * 2 + y // 2
        cp = remote(piece, ib.at[at], s2s.at[k], s2r.at[at], rd, cd)
        here = pltpu.make_async_copy(piece, ib.at[at], s2r.at[at])

        @pl.when(jnp.logical_not(own))
        def _():
            cp.start()

        @pl.when(own)
        def _():
            here.start()

        last.append((cp, own))

    froms = ((r, o), (r ^ 2, h), (r ^ 2, o))
    for k in range(3):
        at = 2 * froms[k][0] + froms[k][1]
        ref = ub.at[at]
        arrived(ref, cr.at[k])
        if k == 0:
            send(ref, ref, cs.at[2], cr.at[2], r ^ 2, c)
        send(ref, ref, ds_.at[k], dr.at[k], r ^ 1, c)
        update_rows(*froms[k])
        if k < 2:
            rs, hs = froms[k][0] ^ 1, froms[k][1]
            arrived(ub.at[2 * rs + hs], dr.at[k])
            update_rows(rs, hs)
        if k == 1:
            for j in range(4):
                arrived(ib.at[j], s2r.at[j])
            ig_ref[...] = (
                (ib[0].astype(F32) + ib[1].astype(F32)) + (ib[2].astype(F32) + ib[3].astype(F32))
            ).astype(BF16)
    arrived(ub.at[2 * (r ^ 3) + o], dr.at[2])
    update_rows(r ^ 3, o)

    for cp, own in last:
        @pl.when(jnp.logical_not(own))
        def _():
            cp.wait_send()
    for cp in others:
        cp.wait_send()


def ortho_scatter_call(grad, momentum, terms, weight):
    vm = pl.BlockSpec(memory_space=pltpu.VMEM)
    dma = pltpu.SemaphoreType.DMA
    return pl.pallas_call(
        ortho_scatter_kernel,
        out_shape=(
            jax.ShapeDtypeStruct((BR, BC), F32),
            jax.ShapeDtypeStruct((BR, BC), BF16),
            jax.ShapeDtypeStruct((FEAT, TOK), BF16),
            jax.ShapeDtypeStruct(weight.shape, BF16),
        ),
        in_specs=[vm, vm, vm, pl.BlockSpec(memory_space=pltpu.HBM)],
        out_specs=(vm, vm, vm, vm),
        scratch_shapes=[
            pltpu.VMEM((8, BC), F32),
            pltpu.VMEM((2, BR, BR), BF16),
            pltpu.VMEM((BR, BC), BF16),
            pltpu.VMEM((3, BR // 2, TOK), BF16),
            pltpu.VMEM((3, BR // 2, TOK), BF16),
            pltpu.VMEM((BR, TOK), BF16),
            pltpu.VMEM((4, FEAT, TOK), BF16),
            pltpu.VMEM((8, BR, HALF), BF16),
            dma((2, 3)), dma((2, 3)), dma((3,)), dma((3,)), dma((4,)), dma((4,)),
            dma((4,)), dma((4,)), dma((2,)),
        ],
        compiler_params=pltpu.CompilerParams(
            collective_id=1, has_side_effects=True, vmem_limit_bytes=34_000_000
        ),
        cost_estimate=pl.CostEstimate(flops=7_000_000_000, bytes_accessed=20_000_000, transcendentals=0),
        name="ortho_scatter",
    )(grad, momentum, terms, weight)


def body(tokens, cotangent, weight, momentum):
    grad, terms = gather_call(tokens.T, cotangent, weight)
    new_momentum, xmat, input_grad, new_weight = ortho_scatter_call(grad, momentum[0], terms, weight)
    update = 32.0 * xmat.astype(F32)
    return new_weight, input_grad.T, new_momentum[None], update[None]


def solution(mesh):
    in_specs = (P("rows", "cols"), P("rows", "cols"), P(None, "cols"), P(("rows", "cols"), None, None))
    out_specs = (
        P(None, "cols"),
        P("rows", "cols"),
        P(("rows", "cols"), None, None),
        P(("rows", "cols"), None, None),
    )
    return jax.shard_map(body, mesh=mesh, in_specs=in_specs, out_specs=out_specs, check_vma=False)
```

```python
import functools

import jax
import jax.numpy as jnp
from jax import lax
from jax.experimental import pallas as pl
from jax.experimental.pallas import tpu as pltpu
from jax.sharding import PartitionSpec as P

NS_STEPS = 2
TOK = 512
FEAT = 192
BR = 768
BC = 1024
HALF = 512
COEF_A = 3.4445
COEF_B = -4.775
COEF_C = 2.0315
BETA = 0.95

MESH = pl.DeviceIdType.MESH
F32 = jnp.float32
BF16 = jnp.bfloat16


def place():
    r = lax.axis_index("rows")
    c = lax.axis_index("cols")
    return r, c, c // 8, (c // 4) % 2, c % 4


def remote(src, dst, send, recv, r, c):
    return pltpu.make_async_remote_copy(
        src_ref=src,
        dst_ref=dst,
        send_sem=send,
        recv_sem=recv,
        device_id=(r, c),
        device_id_type=MESH,
    )


def flip(v):
    return (v % 2) * 2 + v // 2


def group_at(x, r):
    return flip((x + 4 - r) % 4)


def spread_targets():
    r, c, x, zl, y = place()
    out = []
    for zd in range(2):
        for yb in range(2):
            col = ((x + flip(r)) % 4) * 8 + zd * 4 + zl + 2 * yb
            out.append((x, col, (x == r) & (col == c)))
    return out


def spread_sources():
    r, c, x, zl, y = place()
    group = group_at(x, r)
    base = r * 8 + (y % 2) * 4
    return [(group, base + k, (group == r) & (base + k == c)) for k in range(4)]


def x_neighbours():
    r, c, x, zl, y = place()
    low = c % 8
    return ((x + 3) % 4) * 8 + low, ((x + 1) % 4) * 8 + low


def signal_unless(flag, barrier, r, c):
    @pl.when(jnp.logical_not(flag))
    def _():
        pl.semaphore_signal(barrier, inc=1, device_id=(r, c), device_id_type=MESH)


def entry_barrier():
    r, c, x, zl, y = place()
    left, right = x_neighbours()
    barrier = pltpu.get_barrier_semaphore()
    for rd, cd in ((r, left), (r, right), (r ^ 2, c), (r, c ^ 1), (r ^ 1, c)):
        pl.semaphore_signal(barrier, inc=1, device_id=(rd, cd), device_id_type=MESH)
    targets, sources = spread_targets(), spread_sources()
    for rd, cd, own in targets + sources:
        signal_unless(own, barrier, rd, cd)
    own_count = sum(jnp.where(own, 1, 0) for _, _, own in targets + sources)
    pl.semaphore_wait(barrier, 13 - own_count)


def rows_of(group):
    return pl.ds(pl.multiple_of(group * TOK, TOK), TOK)


def half_of(which):
    return pl.ds(pl.multiple_of(which * HALF, HALF), HALF)


def arrived(ref, sem):
    pltpu.make_async_copy(ref, ref, sem).wait()


def tiles(step, rows=256):
    def run(i, carry):
        step(pl.ds(pl.multiple_of(i * rows, rows), rows))
        return carry

    lax.fori_loop(0, BR // rows, run, 0)


CH = 3
CR = BR // CH


def chunk(t):
    return pl.ds(t * CR, CR)


def step_kernel(
    tok_ref, cot_ref, w_ref, mom_ref, newm_ref, x_ref, ig_ref, neww_ref,
    tokv, tokg, cotg, wcat, tacc, terms, sq, ab, xb, fl, fr, sb, ib, ub,
    s1s, s1r, xs, xr, cs, cr, ds_, dr, ws, wr, ls,
    ps, pr, us, ur, vs, vr, s2s, s2r,
):
    r, c, x, zl, y = place()
    h = c % 2
    o = 1 - h
    left, right = x_neighbours()
    mine = cotg.at[rows_of(r), half_of(h)]
    own_tok = pltpu.make_async_copy(tok_ref, tokv, ls.at[0])
    own_cot = pltpu.make_async_copy(cot_ref, mine, ls.at[1])
    own_w = pltpu.make_async_copy(
        w_ref.at[pl.ds(pl.multiple_of((2 * r + h) * BR, BR), BR), :], wcat.at[:, half_of(h)], ls.at[2]
    )
    load_m = pltpu.make_async_copy(mom_ref, newm_ref, ls.at[3])
    load_w = pltpu.make_async_copy(w_ref, neww_ref, ls.at[4])
    for cp in (own_tok, own_cot, own_w, load_m, load_w):
        cp.start()
    entry_barrier()
    own_tok.wait()

    def send_spread(pairs, make):
        out = []
        for k, (rd, cd, own) in enumerate(pairs):
            cp, here = make(k, rd, cd)

            @pl.when(jnp.logical_not(own))
            def _():
                cp.start()

            @pl.when(own)
            def _():
                here.start()

            out.append((cp, own))
        return out

    def spread_tokens(k, rd, cd):
        dst = tokg.at[pl.ds(pl.multiple_of(y * FEAT, FEAT), FEAT), rows_of(r)]
        return remote(tokv, dst, s1s.at[k], s1r.at[y], rd, cd), pltpu.make_async_copy(tokv, dst, s1r.at[y])

    spreads = send_spread(spread_targets(), spread_tokens)

    own_cot.wait()
    others = []

    def send(src, dst, ss, rs, rd, cd):
        cp = remote(src, dst, ss, rs, rd, cd)
        cp.start()
        others.append(cp)

    send(mine, mine, cs.at[0], cr.at[0], r, c ^ 1)
    send(mine, mine, cs.at[1], cr.at[1], r ^ 2, c)
    send(mine, mine, ds_.at[3], dr.at[3], r ^ 1, c)

    send(
        w_ref.at[pl.ds(pl.multiple_of((2 * r + o) * BR, BR), BR), :],
        wcat.at[:, half_of(h)], ws.at[0], wr.at[0], r, c ^ 1,
    )

    q0, ql, qr, q2 = (group_at((x + k) % 4, r) for k in (0, 3, 1, 2))
    for k in range(4):
        piece = tokg.at[pl.ds(k * FEAT, FEAT), rows_of(q0)]
        arrived(piece, s1r.at[k])
        send(piece, piece, xs.at[0, k], xr.at[0, k], r, left)
        send(piece, piece, xs.at[1, k], xr.at[1, k], r, right)

    froms = ((r, o), (r ^ 2, h), (r ^ 2, o))

    def pass_on(k):
        ref = cotg.at[rows_of(froms[k][0]), half_of(froms[k][1])]
        arrived(ref, cr.at[k])
        if k == 0:
            send(ref, ref, cs.at[2], cr.at[2], r ^ 2, c)
        send(ref, ref, ds_.at[k], dr.at[k], r ^ 1, c)

    pass_on(0)
    pass_on(1)

    for k in range(2):
        ref = tokg.at[pl.ds(k * FEAT, FEAT), rows_of(ql)]
        arrived(ref, xr.at[1, k])
        send(ref, ref, xs.at[2, k], xr.at[2, k], r, right)
        ref = tokg.at[pl.ds((k + 2) * FEAT, FEAT), rows_of(qr)]
        arrived(ref, xr.at[0, k + 2])
        send(ref, ref, xs.at[2, k + 2], xr.at[2, k + 2], r, left)

    def from_core(k, rs, hs):
        arrived(cotg.at[rows_of(rs), half_of(hs)], dr.at[k])

    own_w.wait()
    from_core(3, r ^ 1, h)
    from_core(1, r ^ 3, h)
    nt = (((1,), (1,)), ((), ()))

    def terms_half(which, group, first):
        def tile(rows):
            part = lax.dot_general(
                wcat[rows, half_of(which)], cotg[rows_of(group), half_of(which)], nt,
                preferred_element_type=F32,
            )
            if first:
                tacc[rows, rows_of(group)] = part
            else:
                terms[rows, rows_of(group)] = (tacc[rows, rows_of(group)] + part).astype(BF16)

        tiles(tile)

    def all_first(group, carry):
        terms_half(h, group, True)
        return carry

    lax.fori_loop(0, 4, all_first, 0)
    pass_on(2)
    from_core(0, r ^ 1, o)
    from_core(2, r ^ 3, o)

    load_m.wait()
    sq[...] = jnp.zeros_like(sq)

    def grad_step(group, first=False, last=False):
        def tile(rows):
            part = jnp.dot(tokg[rows, rows_of(group)], cotg[rows_of(group), :], preferred_element_type=F32)
            old = newm_ref[rows, :]
            new = (BETA * old if first else old) + part
            newm_ref[rows, :] = new
            if last:
                sq[...] += jnp.sum((new * new).reshape(-1, 8, BC), axis=0)

        tiles(tile)

    grad_step(q0, first=True)
    for k in range(2):
        arrived(tokg.at[pl.ds(k * FEAT, FEAT), rows_of(qr)], xr.at[0, k])
        arrived(tokg.at[pl.ds((k + 2) * FEAT, FEAT), rows_of(ql)], xr.at[1, k + 2])
    grad_step(ql)
    grad_step(qr)
    arrived(wcat.at[:, half_of(o)], wr.at[0])

    MID = BR // 2
    top, low = pl.ds(0, MID), pl.ds(MID, MID)
    terms_half(o, q2, False)
    terms_half(o, qr, False)
    send(terms.at[top, rows_of(q2)], fl.at[0], ps.at[0, 0], pr.at[0, 0], r, right)
    send(terms.at[low, rows_of(q2)], fr.at[0], ps.at[1, 0], pr.at[1, 0], r, left)
    terms_half(o, ql, False)
    send(terms.at[low, rows_of(qr)], fl.at[2], ps.at[0, 1], pr.at[0, 1], r, right)
    terms_half(o, q0, False)
    send(terms.at[top, rows_of(ql)], fr.at[2], ps.at[1, 1], pr.at[1, 1], r, left)
    for k in range(4):
        arrived(tokg.at[pl.ds(k * FEAT, FEAT), rows_of(q2)], xr.at[2, k])
    grad_step(q2, last=True)

    def join(src, base, group):
        def step(i, carry):
            part = pl.ds(pl.multiple_of(i * 64, 64), 64)
            here = pl.ds(pl.multiple_of(base + i * 64, 64), 64)
            src[0, part, :] = (
                src[0, part, :].astype(F32) + terms[here, rows_of(group)].astype(F32)
            ).astype(BF16)
            return carry

        lax.fori_loop(0, MID // 64, step, 0)

    def join_both():
        arrived(fl.at[0], pr.at[0, 0])
        arrived(fr.at[0], pr.at[1, 0])
        join(fl, 0, qr)
        join(fr, MID, ql)
        send(fl.at[0], fl.at[1], ps.at[0, 2], pr.at[0, 2], r, right)
        send(fr.at[0], fr.at[1], ps.at[1, 2], pr.at[1, 2], r, left)

    inverse = 1.0 / (jnp.sqrt(jnp.sum(sq[...])) + 1e-07)

    def scaled(rows):
        x_ref[rows, :] = (newm_ref[rows, :] * inverse).astype(BF16)

    tiles(scaled, 64)

    def send_update(t):
        rows = chunk(t)
        slot = ub.at[2 * r + h, rows, :]
        send(x_ref.at[rows, half_of(o)], slot, us.at[0, t], ur.at[0, t], r, c ^ 1)
        send(x_ref.at[rows, half_of(h)], slot, us.at[1, t], ur.at[1, t], r ^ 2, c)
        send(x_ref.at[rows, half_of(h)], slot, vs.at[3, t], vr.at[3, t], r ^ 1, c)

    def update_rows(rs, hs, t, own=False):
        at = 2 * rs + hs

        def step(i, carry):
            part = pl.ds(pl.multiple_of(t * CR + i * 64, 64), 64)
            here = pl.ds(pl.multiple_of(at * BR + t * CR + i * 64, 64), 64)
            new = x_ref[part, half_of(h)] if own else ub[at, part, :]
            neww_ref[here, :] = (neww_ref[here, :].astype(F32) - 8.0 * new.astype(F32)).astype(BF16)
            return carry

        lax.fori_loop(0, CR // 64, step, 0)

    load_w.wait()
    src, dst = x_ref, xb
    for step in range(NS_STEPS):
        def gram(rows):
            ab[0, rows, :] = lax.dot_general(src[rows, :], src[...], nt, preferred_element_type=F32).astype(BF16)

        def poly(rows):
            a = ab[0, rows, :]
            aa = jnp.dot(a, ab[0], preferred_element_type=F32)
            ab[1, rows, :] = (COEF_B * a.astype(F32) + COEF_C * aa).astype(BF16)

        def apply(rows):
            bx = jnp.dot(ab[1, rows, :], src[...], preferred_element_type=F32)
            dst[rows, :] = (COEF_A * src[rows, :].astype(F32) + bx).astype(BF16)

        tiles(gram)
        tiles(poly)
        if step == 0:
            tiles(apply)
            join_both()
        else:
            apply(chunk(0))
            apply(chunk(1))
            send_update(0)
            apply(chunk(2))
            send_update(1)
            update_rows(r, h, 0, own=True)
            send_update(2)
        src, dst = dst, src

    update_rows(r, h, 1, own=True)
    update_rows(r, h, 2, own=True)

    for ref, i, j in ((fl, 0, 1), (fr, 1, 1), (fl, 0, 2), (fr, 1, 2)):
        arrived(ref.at[3 - j], pr.at[i, j])

    def total(i, carry):
        part = pl.ds(pl.multiple_of(i * 64, 64), 64)
        below = pl.ds(pl.multiple_of(MID + i * 64, 64), 64)
        sb[part, :] = (
            terms[part, rows_of(q0)].astype(F32) + fl[1, part, :].astype(F32) + fr[2, part, :].astype(F32)
        ).astype(BF16)
        sb[below, :] = (
            terms[below, rows_of(q0)].astype(F32) + fr[1, part, :].astype(F32) + fl[2, part, :].astype(F32)
        ).astype(BF16)
        return carry

    lax.fori_loop(0, MID // 64, total, 0)

    def spread_sums(k, rd, cd):
        piece = sb.at[pl.ds(k * FEAT, FEAT), :]
        at = zl * 2 + y // 2
        return (
            remote(piece, ib.at[at], s2s.at[k], s2r.at[at], rd, cd),
            pltpu.make_async_copy(piece, ib.at[at], s2r.at[at]),
        )

    def relay(k, t):
        ref = ub.at[2 * froms[k][0] + froms[k][1], chunk(t), :]
        arrived(ref, ur.at[k, t])
        if k == 0:
            send(ref, ref, us.at[2, t], ur.at[2, t], r ^ 2, c)
        send(ref, ref, vs.at[k, t], vr.at[k, t], r ^ 1, c)

    def core_rows(k, t):
        rs, hs = (froms[k][0] ^ 1, froms[k][1]) if k < 3 else (r ^ 1, h)
        arrived(ub.at[2 * rs + hs, chunk(t), :], vr.at[k, t])
        update_rows(rs, hs, t)

    spreads += send_spread(spread_sources(), spread_sums)
    for t in range(CH):
        relay(0, t)
        relay(1, t)
    for t in range(CH):
        core_rows(3, t)
        update_rows(*froms[0], t)
        update_rows(*froms[1], t)
        core_rows(0, t)
        core_rows(1, t)
    for j in range(4):
        arrived(ib.at[j], s2r.at[j])
    ig_ref[...] = (
        (ib[0].astype(F32) + ib[1].astype(F32)) + (ib[2].astype(F32) + ib[3].astype(F32))
    ).astype(BF16)
    for t in range(CH):
        relay(2, t)
        update_rows(*froms[2], t)
        core_rows(2, t)

    for cp, own in spreads:
        @pl.when(jnp.logical_not(own))
        def _():
            cp.wait_send()
    for cp in others:
        cp.wait_send()


def step_call(tok, cot, weight, momentum):
    hbm = pl.BlockSpec(memory_space=pltpu.HBM)
    vm = pl.BlockSpec(memory_space=pltpu.VMEM)
    dma = pltpu.SemaphoreType.DMA
    return pl.pallas_call(
        step_kernel,
        out_shape=(
            jax.ShapeDtypeStruct((BR, BC), F32),
            jax.ShapeDtypeStruct((BR, BC), BF16),
            jax.ShapeDtypeStruct((FEAT, TOK), BF16),
            jax.ShapeDtypeStruct(weight.shape, BF16),
        ),
        in_specs=[hbm, hbm, hbm, hbm],
        out_specs=(vm, vm, vm, vm),
        scratch_shapes=[
            pltpu.VMEM((FEAT, TOK), BF16),
            pltpu.VMEM((BR, 4 * TOK), BF16),
            pltpu.VMEM((4 * TOK, BC), BF16),
            pltpu.VMEM((BR, BC), BF16),
            pltpu.VMEM((BR, 4 * TOK), F32),
            pltpu.VMEM((BR, 4 * TOK), BF16),
            pltpu.VMEM((8, BC), F32),
            pltpu.VMEM((2, BR, BR), BF16),
            pltpu.VMEM((BR, BC), BF16),
            pltpu.VMEM((3, BR // 2, TOK), BF16),
            pltpu.VMEM((3, BR // 2, TOK), BF16),
            pltpu.VMEM((BR, TOK), BF16),
            pltpu.VMEM((4, FEAT, TOK), BF16),
            pltpu.VMEM((8, BR, HALF), BF16),
            dma((4,)), dma((4,)), dma((3, 4)), dma((3, 4)), dma((3,)), dma((3,)),
            dma((4,)), dma((4,)), dma((1,)), dma((1,)), dma((5,)),
            dma((2, 3)), dma((2, 3)), dma((3, CH)), dma((3, CH)), dma((4, CH)), dma((4, CH)),
            dma((4,)), dma((4,)),
        ],
        compiler_params=pltpu.CompilerParams(
            collective_id=0, has_side_effects=True, vmem_limit_bytes=40_000_000
        ),
        cost_estimate=pl.CostEstimate(flops=14_000_000_000, bytes_accessed=20_000_000, transcendentals=0),
        name="step",
    )(tok, cot, weight, momentum)


def write_kernel(newm_ref, x_ref, ig_ref, neww_ref, newm_out, upd_out, ig_out, neww_out, buf, sem):
    copies = [
        pltpu.make_async_copy(neww_ref, neww_out, sem.at[0]),
        pltpu.make_async_copy(newm_ref, newm_out, sem.at[1]),
        pltpu.make_async_copy(ig_ref, ig_out, sem.at[2]),
    ]
    for cp in copies:
        cp.start()
    for t in range(CH):
        buf[chunk(t), :] = 32.0 * x_ref[chunk(t), :].astype(F32)
        cp = pltpu.make_async_copy(buf.at[chunk(t), :], upd_out.at[chunk(t), :], sem.at[3 + t])
        cp.start()
        copies.append(cp)
    for cp in copies:
        cp.wait()


def write_call(newm, xmat, ig, neww):
    hbm = pl.BlockSpec(memory_space=pltpu.HBM)
    vm = pl.BlockSpec(memory_space=pltpu.VMEM)
    return pl.pallas_call(
        write_kernel,
        out_shape=(
            jax.ShapeDtypeStruct(newm.shape, F32),
            jax.ShapeDtypeStruct(xmat.shape, F32),
            jax.ShapeDtypeStruct(ig.shape, BF16),
            jax.ShapeDtypeStruct(neww.shape, BF16),
        ),
        in_specs=[vm, vm, vm, vm],
        out_specs=(hbm, hbm, hbm, hbm),
        scratch_shapes=[pltpu.VMEM((BR, BC), F32), pltpu.SemaphoreType.DMA((3 + CH,))],
        compiler_params=pltpu.CompilerParams(vmem_limit_bytes=20_000_000),
        cost_estimate=pl.CostEstimate(flops=1_000_000, bytes_accessed=13_000_000, transcendentals=0),
        name="write_out",
    )(newm, xmat, ig, neww)


def body(tokens, cotangent, weight, momentum):
    pin = lambda a: pltpu.with_memory_space_constraint(a, pltpu.HBM)
    results = step_call(pin(tokens.T), pin(cotangent), pin(weight), pin(momentum[0]))
    new_momentum, update, input_grad, new_weight = write_call(*results)
    return new_weight, input_grad.T, new_momentum[None], update[None]


def solution(mesh):
    in_specs = (P("rows", "cols"), P("rows", "cols"), P(None, "cols"), P(("rows", "cols"), None, None))
    out_specs = (
        P(None, "cols"),
        P("rows", "cols"),
        P(("rows", "cols"), None, None),
        P(("rows", "cols"), None, None),
    )
    return jax.shard_map(body, mesh=mesh, in_specs=in_specs, out_specs=out_specs, check_vma=False)
```

```python
import functools

import jax
import jax.numpy as jnp
from jax import lax
from jax.experimental import pallas as pl
from jax.experimental.pallas import tpu as pltpu
from jax.sharding import PartitionSpec as P

NS_STEPS = 2
TOK = 512
FEAT = 192
BR = 768
BC = 1024
HALF = 512
COEF_A = 3.4445
COEF_B = -4.775
COEF_C = 2.0315
BETA = 0.95

MESH = pl.DeviceIdType.MESH
F32 = jnp.float32
BF16 = jnp.bfloat16


def place():
    r = lax.axis_index("rows")
    c = lax.axis_index("cols")
    return r, c, c // 8, (c // 4) % 2, c % 4


def remote(src, dst, send, recv, r, c):
    return pltpu.make_async_remote_copy(
        src_ref=src,
        dst_ref=dst,
        send_sem=send,
        recv_sem=recv,
        device_id=(r, c),
        device_id_type=MESH,
    )


def flip(v):
    return (v % 2) * 2 + v // 2


def group_at(x, r):
    return flip((x + 4 - r) % 4)


def spread_targets():
    r, c, x, zl, y = place()
    base = ((x + flip(r)) % 4) * 8 + zl + 2 * (y // 2)
    return [(x, base + 4 * k, (x == r) & (base + 4 * k == c)) for k in range(2)]


def spread_sources():
    r, c, x, zl, y = place()
    group = group_at(x, r)
    base = r * 8 + (y % 2) * 4 + 2 * (y // 2)
    return [(group, base + k, (group == r) & (base + k == c)) for k in range(2)]


def x_neighbours():
    r, c, x, zl, y = place()
    low = c % 8
    return ((x + 3) % 4) * 8 + low, ((x + 1) % 4) * 8 + low


def signal_unless(flag, barrier, r, c):
    @pl.when(jnp.logical_not(flag))
    def _():
        pl.semaphore_signal(barrier, inc=1, device_id=(r, c), device_id_type=MESH)


def entry_barrier():
    r, c, x, zl, y = place()
    left, right = x_neighbours()
    barrier = pltpu.get_barrier_semaphore()
    for rd, cd in ((r, left), (r, right), (r ^ 2, c), (r, c ^ 1), (r, c ^ 2), (r ^ 1, c)):
        pl.semaphore_signal(barrier, inc=1, device_id=(rd, cd), device_id_type=MESH)
    targets, sources = spread_targets(), spread_sources()
    for rd, cd, own in targets + sources:
        signal_unless(own, barrier, rd, cd)
    own_count = sum(jnp.where(own, 1, 0) for _, _, own in targets + sources)
    pl.semaphore_wait(barrier, 10 - own_count)


def rows_of(group):
    return pl.ds(pl.multiple_of(group * TOK, TOK), TOK)


def half_of(which):
    return pl.ds(pl.multiple_of(which * HALF, HALF), HALF)


def arrived(ref, sem):
    pltpu.make_async_copy(ref, ref, sem).wait()


def tiles(step, rows=256):
    def run(i, carry):
        step(pl.ds(pl.multiple_of(i * rows, rows), rows))
        return carry

    lax.fori_loop(0, BR // rows, run, 0)


CH = 3
CR = BR // CH


def chunk(t):
    return pl.ds(t * CR, CR)


def step_kernel(
    tok_ref, cot_ref, w_ref, mom_ref, newm_ref, x_ref, ig_ref, neww_ref,
    tokv, tokg, cotg, wcat, tacc, terms, sq, ab, xb, fl, fr, sb, sp, ib, ub,
    s1s, s1r, xs, xr, cs, cr, ds_, dr, ws, wr, ls,
    ps, pr, us, ur, vs, vr, s2s, s2r,
):
    r, c, x, zl, y = place()
    h = c % 2
    o = 1 - h
    left, right = x_neighbours()
    mine = cotg.at[rows_of(r), half_of(h)]
    own_tok = pltpu.make_async_copy(tok_ref, tokv, ls.at[0])
    own_cot = pltpu.make_async_copy(cot_ref, mine, ls.at[1])
    own_w = pltpu.make_async_copy(
        w_ref.at[pl.ds(pl.multiple_of((2 * r + h) * BR, BR), BR), :], wcat.at[:, half_of(h)], ls.at[2]
    )
    load_m = pltpu.make_async_copy(mom_ref, newm_ref, ls.at[3])
    load_w = pltpu.make_async_copy(w_ref, neww_ref, ls.at[4])
    for cp in (own_tok, own_cot, own_w, load_m, load_w):
        cp.start()
    entry_barrier()
    own_tok.wait()

    def send_spread(pairs, make):
        out = []
        for k, (rd, cd, own) in enumerate(pairs):
            cp, here = make(k, rd, cd)

            @pl.when(jnp.logical_not(own))
            def _():
                cp.start()

            @pl.when(own)
            def _():
                here.start()

            out.append((cp, own))
        return out

    def spread_tokens(k, rd, cd):
        dst = tokg.at[pl.ds(pl.multiple_of(y * FEAT, FEAT), FEAT), rows_of(r)]
        got = s1r.at[y % 2]
        return remote(tokv, dst, s1s.at[k], got, rd, cd), pltpu.make_async_copy(tokv, dst, got)

    spreads = send_spread(spread_targets(), spread_tokens)

    own_cot.wait()
    others = []

    def send(src, dst, ss, rs, rd, cd):
        cp = remote(src, dst, ss, rs, rd, cd)
        cp.start()
        others.append(cp)

    send(mine, mine, cs.at[0], cr.at[0], r, c ^ 1)
    send(mine, mine, cs.at[1], cr.at[1], r ^ 2, c)
    send(mine, mine, ds_.at[3], dr.at[3], r ^ 1, c)

    q0, ql, qr, q2 = (group_at((x + k) % 4, r) for k in (0, 3, 1, 2))
    yb = y // 2

    def piece(j, group):
        at = (2 * yb + j) % 4
        return tokg.at[pl.ds(pl.multiple_of(at * FEAT, FEAT), FEAT), rows_of(group)]

    def round_x(j):
        ref = piece(j, q0)
        arrived(ref, s1r.at[j])
        if j < 2:
            send(ref, ref, s1s.at[2 + j], s1r.at[2 + j], r, c ^ 2)
        send(ref, ref, xs.at[0, j], xr.at[0, j], r, left)
        send(ref, ref, xs.at[1, j], xr.at[1, j], r, right)

    round_x(0)
    round_x(1)

    send(
        w_ref.at[pl.ds(pl.multiple_of((2 * r + o) * BR, BR), BR), :],
        wcat.at[:, half_of(h)], ws.at[0], wr.at[0], r, c ^ 1,
    )

    froms = ((r, o), (r ^ 2, h), (r ^ 2, o))

    def pass_on(k):
        ref = cotg.at[rows_of(froms[k][0]), half_of(froms[k][1])]
        arrived(ref, cr.at[k])
        if k == 0:
            send(ref, ref, cs.at[2], cr.at[2], r ^ 2, c)
        send(ref, ref, ds_.at[k], dr.at[k], r ^ 1, c)

    pass_on(0)
    round_x(2)
    round_x(3)
    pass_on(1)

    for j in range(4):
        came, group, to = ((1, ql, right), (0, qr, left))[j % 2]
        ref = piece(j, group)
        arrived(ref, xr.at[came, j])
        send(ref, ref, xs.at[2, j], xr.at[2, j], r, to)

    def from_core(k, rs, hs):
        arrived(cotg.at[rows_of(rs), half_of(hs)], dr.at[k])

    own_w.wait()
    from_core(3, r ^ 1, h)
    from_core(1, r ^ 3, h)
    nt = (((1,), (1,)), ((), ()))

    def terms_half(which, group, first):
        def tile(rows):
            part = lax.dot_general(
                wcat[rows, half_of(which)], cotg[rows_of(group), half_of(which)], nt,
                preferred_element_type=F32,
            )
            if first:
                tacc[rows, rows_of(group)] = part
            else:
                terms[rows, rows_of(group)] = (tacc[rows, rows_of(group)] + part).astype(BF16)

        tiles(tile)

    def all_first(group, carry):
        terms_half(h, group, True)
        return carry

    lax.fori_loop(0, 4, all_first, 0)
    pass_on(2)
    from_core(0, r ^ 1, o)
    from_core(2, r ^ 3, o)

    load_m.wait()
    sq[...] = jnp.zeros_like(sq)

    def grad_step(group, first=False, last=False):
        def tile(rows):
            part = jnp.dot(tokg[rows, rows_of(group)], cotg[rows_of(group), :], preferred_element_type=F32)
            old = newm_ref[rows, :]
            new = (BETA * old if first else old) + part
            newm_ref[rows, :] = new
            if last:
                sq[...] += jnp.sum((new * new).reshape(-1, 8, BC), axis=0)

        tiles(tile)

    grad_step(q0, first=True)
    for j in range(4):
        came, group = ((0, qr), (1, ql))[j % 2]
        arrived(piece(j, group), xr.at[came, j])
    grad_step(ql)
    grad_step(qr)
    for j in range(4):
        arrived(piece(j, q2), xr.at[2, j])
    grad_step(q2, last=True)

    MID = BR // 2
    top, low = pl.ds(0, MID), pl.ds(MID, MID)

    def join(src, base, group):
        def step(i, carry):
            part = pl.ds(pl.multiple_of(i * 64, 64), 64)
            here = pl.ds(pl.multiple_of(base + i * 64, 64), 64)
            src[0, part, :] = (
                src[0, part, :].astype(F32) + terms[here, rows_of(group)].astype(F32)
            ).astype(BF16)
            return carry

        lax.fori_loop(0, MID // 64, step, 0)

    def join_both():
        arrived(fl.at[0], pr.at[0, 0])
        arrived(fr.at[0], pr.at[1, 0])
        join(fl, 0, qr)
        join(fr, MID, ql)
        send(fl.at[0], fl.at[1], ps.at[0, 2], pr.at[0, 2], r, right)
        send(fr.at[0], fr.at[1], ps.at[1, 2], pr.at[1, 2], r, left)

    inverse = 1.0 / (jnp.sqrt(jnp.sum(sq[...])) + 1e-07)

    def scaled(rows):
        x_ref[rows, :] = (newm_ref[rows, :] * inverse).astype(BF16)

    tiles(scaled, 64)

    def start_sums():
        arrived(wcat.at[:, half_of(o)], wr.at[0])
        terms_half(o, q2, False)
        terms_half(o, qr, False)
        send(terms.at[top, rows_of(q2)], fl.at[0], ps.at[0, 0], pr.at[0, 0], r, right)
        send(terms.at[low, rows_of(q2)], fr.at[0], ps.at[1, 0], pr.at[1, 0], r, left)
        terms_half(o, ql, False)
        send(terms.at[low, rows_of(qr)], fl.at[2], ps.at[0, 1], pr.at[0, 1], r, right)
        terms_half(o, q0, False)
        send(terms.at[top, rows_of(ql)], fr.at[2], ps.at[1, 1], pr.at[1, 1], r, left)

    def send_update(t):
        rows = chunk(t)
        slot = ub.at[2 * r + h, rows, :]
        send(x_ref.at[rows, half_of(o)], slot, us.at[0, t], ur.at[0, t], r, c ^ 1)
        send(x_ref.at[rows, half_of(h)], slot, us.at[1, t], ur.at[1, t], r ^ 2, c)
        send(x_ref.at[rows, half_of(h)], slot, vs.at[3, t], vr.at[3, t], r ^ 1, c)

    def update_rows(rs, hs, t, own=False):
        at = 2 * rs + hs

        def step(i, carry):
            part = pl.ds(pl.multiple_of(t * CR + i * 64, 64), 64)
            here = pl.ds(pl.multiple_of(at * BR + t * CR + i * 64, 64), 64)
            new = x_ref[part, half_of(h)] if own else ub[at, part, :]
            neww_ref[here, :] = (neww_ref[here, :].astype(F32) - 8.0 * new.astype(F32)).astype(BF16)
            return carry

        lax.fori_loop(0, CR // 64, step, 0)

    load_w.wait()
    src, dst = x_ref, xb
    for step in range(NS_STEPS):
        def gram(rows):
            ab[0, rows, :] = lax.dot_general(src[rows, :], src[...], nt, preferred_element_type=F32).astype(BF16)

        def poly(rows):
            a = ab[0, rows, :]
            aa = jnp.dot(a, ab[0], preferred_element_type=F32)
            ab[1, rows, :] = (COEF_B * a.astype(F32) + COEF_C * aa).astype(BF16)

        def apply(rows):
            bx = jnp.dot(ab[1, rows, :], src[...], preferred_element_type=F32)
            dst[rows, :] = (COEF_A * src[rows, :].astype(F32) + bx).astype(BF16)

        tiles(gram)
        tiles(poly)
        if step == 0:
            start_sums()
            tiles(apply)
        else:
            apply(chunk(0))
            apply(chunk(1))
            send_update(0)
            apply(chunk(2))
            send_update(1)
            update_rows(r, h, 0, own=True)
            send_update(2)
        src, dst = dst, src

    update_rows(r, h, 1, own=True)
    update_rows(r, h, 2, own=True)
    join_both()

    def total(i, carry):
        part = pl.ds(pl.multiple_of(i * 64, 64), 64)
        below = pl.ds(pl.multiple_of(MID + i * 64, 64), 64)
        sb[part, :] = (
            terms[part, rows_of(q0)].astype(F32) + fl[1, part, :].astype(F32) + fr[2, part, :].astype(F32)
        ).astype(BF16)
        sb[below, :] = (
            terms[below, rows_of(q0)].astype(F32) + fr[1, part, :].astype(F32) + fl[2, part, :].astype(F32)
        ).astype(BF16)
        return carry

    def pieces_of(which):
        return pl.ds(pl.multiple_of(which * MID, MID), MID)

    def spread_sums(k, rd, cd):
        part = sb.at[pl.ds(pl.multiple_of((2 * yb + k) * FEAT, FEAT), FEAT), :]
        return (
            remote(part, ib.at[zl], s2s.at[k], s2r.at[zl], rd, cd),
            pltpu.make_async_copy(part, ib.at[zl], s2r.at[zl]),
        )

    def pair_sum(i, carry):
        part = pl.ds(pl.multiple_of(i * 64, 64), 64)
        here = pl.ds(pl.multiple_of(yb * MID + i * 64, 64), 64)
        sb[here, :] = (sb[here, :].astype(F32) + sp[part, :].astype(F32)).astype(BF16)
        return carry

    def relay(k, t):
        ref = ub.at[2 * froms[k][0] + froms[k][1], chunk(t), :]
        arrived(ref, ur.at[k, t])
        if k == 0:
            send(ref, ref, us.at[2, t], ur.at[2, t], r ^ 2, c)
        send(ref, ref, vs.at[k, t], vr.at[k, t], r ^ 1, c)

    def core_rows(k, t):
        rs, hs = (froms[k][0] ^ 1, froms[k][1]) if k < 3 else (r ^ 1, h)
        arrived(ub.at[2 * rs + hs, chunk(t), :], vr.at[k, t])
        update_rows(rs, hs, t)

    for t in range(CH):
        relay(0, t)
        relay(1, t)
        core_rows(3, t)
        update_rows(*froms[0], t)
        update_rows(*froms[1], t)

    for ref, i, j in ((fl, 0, 1), (fr, 1, 1), (fl, 0, 2), (fr, 1, 2)):
        arrived(ref.at[3 - j], pr.at[i, j])

    lax.fori_loop(0, MID // 64, total, 0)
    for t in range(CH):
        core_rows(0, t)
    send(sb.at[pieces_of(1 - yb), :], sp, s2s.at[2], s2r.at[2], r, c ^ 2)
    for t in range(CH):
        core_rows(1, t)
    for t in range(CH):
        relay(2, t)
        update_rows(*froms[2], t)
        if t == 0:
            arrived(sp, s2r.at[2])
            lax.fori_loop(0, MID // 64, pair_sum, 0)
            core_rows(2, 0)
            spreads += send_spread(spread_sources(), spread_sums)
        elif t == 1:
            core_rows(2, 1)
        else:
            for j in range(2):
                arrived(ib.at[j], s2r.at[j])
            ig_ref[...] = (ib[0].astype(F32) + ib[1].astype(F32)).astype(BF16)
            core_rows(2, 2)

    for cp, own in spreads:
        @pl.when(jnp.logical_not(own))
        def _():
            cp.wait_send()
    for cp in others:
        cp.wait_send()


def step_call(tok, cot, weight, momentum):
    hbm = pl.BlockSpec(memory_space=pltpu.HBM)
    vm = pl.BlockSpec(memory_space=pltpu.VMEM)
    dma = pltpu.SemaphoreType.DMA
    return pl.pallas_call(
        step_kernel,
        out_shape=(
            jax.ShapeDtypeStruct((BR, BC), F32),
            jax.ShapeDtypeStruct((BR, BC), BF16),
            jax.ShapeDtypeStruct((FEAT, TOK), BF16),
            jax.ShapeDtypeStruct(weight.shape, BF16),
        ),
        in_specs=[hbm, hbm, hbm, hbm],
        out_specs=(vm, vm, vm, vm),
        scratch_shapes=[
            pltpu.VMEM((FEAT, TOK), BF16),
            pltpu.VMEM((BR, 4 * TOK), BF16),
            pltpu.VMEM((4 * TOK, BC), BF16),
            pltpu.VMEM((BR, BC), BF16),
            pltpu.VMEM((BR, 4 * TOK), F32),
            pltpu.VMEM((BR, 4 * TOK), BF16),
            pltpu.VMEM((8, BC), F32),
            pltpu.VMEM((2, BR, BR), BF16),
            pltpu.VMEM((BR, BC), BF16),
            pltpu.VMEM((3, BR // 2, TOK), BF16),
            pltpu.VMEM((3, BR // 2, TOK), BF16),
            pltpu.VMEM((BR, TOK), BF16),
            pltpu.VMEM((BR // 2, TOK), BF16),
            pltpu.VMEM((2, FEAT, TOK), BF16),
            pltpu.VMEM((8, BR, HALF), BF16),
            dma((4,)), dma((4,)), dma((3, 4)), dma((3, 4)), dma((3,)), dma((3,)),
            dma((4,)), dma((4,)), dma((1,)), dma((1,)), dma((5,)),
            dma((2, 3)), dma((2, 3)), dma((3, CH)), dma((3, CH)), dma((4, CH)), dma((4, CH)),
            dma((3,)), dma((3,)),
        ],
        compiler_params=pltpu.CompilerParams(
            collective_id=0, has_side_effects=True, vmem_limit_bytes=40_000_000
        ),
        cost_estimate=pl.CostEstimate(flops=14_000_000_000, bytes_accessed=20_000_000, transcendentals=0),
        name="step",
    )(tok, cot, weight, momentum)


def write_kernel(newm_ref, x_ref, ig_ref, neww_ref, newm_out, upd_out, ig_out, neww_out, buf, sem):
    copies = [
        pltpu.make_async_copy(neww_ref, neww_out, sem.at[0]),
        pltpu.make_async_copy(newm_ref, newm_out, sem.at[1]),
        pltpu.make_async_copy(ig_ref, ig_out, sem.at[2]),
    ]
    for cp in copies:
        cp.start()
    for t in range(CH):
        buf[chunk(t), :] = 32.0 * x_ref[chunk(t), :].astype(F32)
        cp = pltpu.make_async_copy(buf.at[chunk(t), :], upd_out.at[chunk(t), :], sem.at[3 + t])
        cp.start()
        copies.append(cp)
    for cp in copies:
        cp.wait()


def write_call(newm, xmat, ig, neww):
    hbm = pl.BlockSpec(memory_space=pltpu.HBM)
    vm = pl.BlockSpec(memory_space=pltpu.VMEM)
    return pl.pallas_call(
        write_kernel,
        out_shape=(
            jax.ShapeDtypeStruct(newm.shape, F32),
            jax.ShapeDtypeStruct(xmat.shape, F32),
            jax.ShapeDtypeStruct(ig.shape, BF16),
            jax.ShapeDtypeStruct(neww.shape, BF16),
        ),
        in_specs=[vm, vm, vm, vm],
        out_specs=(hbm, hbm, hbm, hbm),
        scratch_shapes=[pltpu.VMEM((BR, BC), F32), pltpu.SemaphoreType.DMA((3 + CH,))],
        compiler_params=pltpu.CompilerParams(vmem_limit_bytes=20_000_000),
        cost_estimate=pl.CostEstimate(flops=1_000_000, bytes_accessed=13_000_000, transcendentals=0),
        name="write_out",
    )(newm, xmat, ig, neww)


def body(tokens, cotangent, weight, momentum):
    pin = lambda a: pltpu.with_memory_space_constraint(a, pltpu.HBM)
    results = step_call(pin(tokens.T), pin(cotangent), pin(weight), pin(momentum[0]))
    new_momentum, update, input_grad, new_weight = write_call(*results)
    return new_weight, input_grad.T, new_momentum[None], update[None]


def solution(mesh):
    in_specs = (P("rows", "cols"), P("rows", "cols"), P(None, "cols"), P(("rows", "cols"), None, None))
    out_specs = (
        P(None, "cols"),
        P("rows", "cols"),
        P(("rows", "cols"), None, None),
        P(("rows", "cols"), None, None),
    )
    return jax.shard_map(body, mesh=mesh, in_specs=in_specs, out_specs=out_specs, check_vma=False)
```

```python
import functools

import jax
import jax.numpy as jnp
from jax import lax
from jax.experimental import pallas as pl
from jax.experimental.pallas import tpu as pltpu
from jax.sharding import PartitionSpec as P

NS_STEPS = 2
TOK = 512
FEAT = 192
BR = 768
BC = 1024
HALF = 512
COEF_A = 3.4445
COEF_B = -4.775
COEF_C = 2.0315
BETA = 0.95

MESH = pl.DeviceIdType.MESH
F32 = jnp.float32
BF16 = jnp.bfloat16


def place():
    r = lax.axis_index("rows")
    c = lax.axis_index("cols")
    return r, c, c // 8, (c // 4) % 2, c % 4


def remote(src, dst, send, recv, r, c):
    return pltpu.make_async_remote_copy(
        src_ref=src,
        dst_ref=dst,
        send_sem=send,
        recv_sem=recv,
        device_id=(r, c),
        device_id_type=MESH,
    )


def flip(v):
    return (v % 2) * 2 + v // 2


def group_at(x, r):
    return flip((x + 4 - r) % 4)


def spread_targets():
    r, c, x, zl, y = place()
    base = ((x + flip(r)) % 4) * 8 + zl + 2 * (y // 2)
    return [(x, base + 4 * k, (x == r) & (base + 4 * k == c)) for k in range(2)]


def spread_sources():
    r, c, x, zl, y = place()
    group = group_at(x, r)
    base = r * 8 + (y % 2) * 4 + 2 * (y // 2)
    return [(group, base + k, (group == r) & (base + k == c)) for k in range(2)]


def x_neighbours():
    r, c, x, zl, y = place()
    low = c % 8
    return ((x + 3) % 4) * 8 + low, ((x + 1) % 4) * 8 + low


def signal_unless(flag, barrier, r, c):
    @pl.when(jnp.logical_not(flag))
    def _():
        pl.semaphore_signal(barrier, inc=1, device_id=(r, c), device_id_type=MESH)


def entry_barrier():
    r, c, x, zl, y = place()
    left, right = x_neighbours()
    barrier = pltpu.get_barrier_semaphore()
    for rd, cd in ((r, left), (r, right), (r ^ 2, c), (r, c ^ 1), (r, c ^ 2), (r ^ 1, c)):
        pl.semaphore_signal(barrier, inc=1, device_id=(rd, cd), device_id_type=MESH)
    targets, sources = spread_targets(), spread_sources()
    for rd, cd, own in targets + sources:
        signal_unless(own, barrier, rd, cd)
    own_count = sum(jnp.where(own, 1, 0) for _, _, own in targets + sources)
    pl.semaphore_wait(barrier, 10 - own_count)


def rows_of(group):
    return pl.ds(pl.multiple_of(group * TOK, TOK), TOK)


def half_of(which):
    return pl.ds(pl.multiple_of(which * HALF, HALF), HALF)


def arrived(ref, sem):
    pltpu.make_async_copy(ref, ref, sem).wait()


def tiles(step, rows=256):
    def run(i, carry):
        step(pl.ds(pl.multiple_of(i * rows, rows), rows))
        return carry

    lax.fori_loop(0, BR // rows, run, 0)


CH = 3
CR = BR // CH


def chunk(t):
    return pl.ds(t * CR, CR)


def step_kernel(
    tok_ref, cot_ref, w_ref, mom_ref, newm_ref, x_ref, ig_ref, neww_ref,
    tokv, tokg, cotg, wcat, tacc, terms, sq, ab, xb, fl, fr, sb, sp, ib, ub,
    s1s, s1r, xs, xr, cs, cr, ds_, dr, ws, wr, ls,
    ps, pr, us, ur, vs, vr, s2s, s2r,
):
    r, c, x, zl, y = place()
    h = c % 2
    o = 1 - h
    left, right = x_neighbours()
    mine = cotg.at[rows_of(r), half_of(h)]
    own_tok = pltpu.make_async_copy(tok_ref, tokv, ls.at[0])
    own_cot = pltpu.make_async_copy(cot_ref, mine, ls.at[1])
    own_w = pltpu.make_async_copy(
        w_ref.at[pl.ds(pl.multiple_of((2 * r + h) * BR, BR), BR), :], wcat.at[:, half_of(h)], ls.at[2]
    )
    load_m = pltpu.make_async_copy(mom_ref, newm_ref, ls.at[3])
    load_w = pltpu.make_async_copy(w_ref, neww_ref, ls.at[4])
    for cp in (own_tok, own_cot, own_w, load_m, load_w):
        cp.start()
    entry_barrier()
    own_tok.wait()

    def send_spread(pairs, make):
        out = []
        for k, (rd, cd, own) in enumerate(pairs):
            cp, here = make(k, rd, cd)

            @pl.when(jnp.logical_not(own))
            def _():
                cp.start()

            @pl.when(own)
            def _():
                here.start()

            out.append((cp, own))
        return out

    def spread_tokens(k, rd, cd):
        dst = tokg.at[pl.ds(pl.multiple_of(y * FEAT, FEAT), FEAT), rows_of(r)]
        got = s1r.at[y % 2]
        return remote(tokv, dst, s1s.at[k], got, rd, cd), pltpu.make_async_copy(tokv, dst, got)

    spreads = send_spread(spread_targets(), spread_tokens)

    own_cot.wait()
    others = []

    def send(src, dst, ss, rs, rd, cd):
        cp = remote(src, dst, ss, rs, rd, cd)
        cp.start()
        others.append(cp)

    send(mine, mine, cs.at[0], cr.at[0], r, c ^ 1)
    send(mine, mine, ds_.at[3], dr.at[3], r ^ 1, c)

    q0, ql, qr, q2 = (group_at((x + k) % 4, r) for k in (0, 3, 1, 2))
    yb = y // 2

    def piece(j, group):
        at = (2 * yb + j) % 4
        return tokg.at[pl.ds(pl.multiple_of(at * FEAT, FEAT), FEAT), rows_of(group)]

    def round_x(j):
        ref = piece(j, q0)
        arrived(ref, s1r.at[j])
        if j < 2:
            send(ref, ref, s1s.at[2 + j], s1r.at[2 + j], r, c ^ 2)
        send(ref, ref, xs.at[0, j], xr.at[0, j], r, left)
        send(ref, ref, xs.at[1, j], xr.at[1, j], r, right)

    round_x(0)
    round_x(1)
    send(mine, mine, cs.at[1], cr.at[1], r ^ 2, c)

    send(
        w_ref.at[pl.ds(pl.multiple_of((2 * r + o) * BR, BR), BR), :],
        wcat.at[:, half_of(h)], ws.at[0], wr.at[0], r, c ^ 1,
    )

    froms = ((r, o), (r ^ 2, h), (r ^ 2, o))

    def pass_on(k):
        ref = cotg.at[rows_of(froms[k][0]), half_of(froms[k][1])]
        arrived(ref, cr.at[k])
        if k == 0:
            send(ref, ref, cs.at[2], cr.at[2], r ^ 2, c)
        send(ref, ref, ds_.at[k], dr.at[k], r ^ 1, c)

    def round_on(j):
        came, group, to = ((1, ql, right), (0, qr, left))[j % 2]
        ref = piece(j, group)
        arrived(ref, xr.at[came, j])
        send(ref, ref, xs.at[2, j], xr.at[2, j], r, to)

    pass_on(0)
    round_on(0)
    round_on(1)
    round_x(2)
    round_x(3)
    pass_on(1)

    def from_core(k, rs, hs):
        arrived(cotg.at[rows_of(rs), half_of(hs)], dr.at[k])

    own_w.wait()
    from_core(3, r ^ 1, h)
    from_core(1, r ^ 3, h)
    nt = (((1,), (1,)), ((), ()))

    def terms_half(which, group, first):
        def tile(rows):
            part = lax.dot_general(
                wcat[rows, half_of(which)], cotg[rows_of(group), half_of(which)], nt,
                preferred_element_type=F32,
            )
            if first:
                tacc[rows, rows_of(group)] = part
            else:
                terms[rows, rows_of(group)] = (tacc[rows, rows_of(group)] + part).astype(BF16)

        tiles(tile)

    def all_first(group, carry):
        terms_half(h, group, True)
        return carry

    lax.fori_loop(0, 4, all_first, 0)
    round_on(2)
    round_on(3)

    load_m.wait()
    sq[...] = jnp.zeros_like(sq)

    def grad_step(group, which, first=False, last=False):
        def tile(rows):
            part = jnp.dot(
                tokg[rows, rows_of(group)], cotg[rows_of(group), half_of(which)], preferred_element_type=F32
            )
            old = newm_ref[rows, half_of(which)]
            new = (BETA * old if first else old) + part
            newm_ref[rows, half_of(which)] = new
            if last:
                sq[...] += jnp.sum((new * new).reshape(-1, 8, HALF), axis=0)

        tiles(tile)

    pass_on(2)
    grad_step(q0, h, first=True)
    for j in range(4):
        came, group = ((0, qr), (1, ql))[j % 2]
        arrived(piece(j, group), xr.at[came, j])
    grad_step(ql, h)
    grad_step(qr, h)
    from_core(0, r ^ 1, o)
    from_core(2, r ^ 3, o)
    grad_step(q0, o, first=True)
    grad_step(ql, o)
    grad_step(qr, o)
    for j in range(4):
        arrived(piece(j, q2), xr.at[2, j])
    grad_step(q2, h, last=True)
    grad_step(q2, o, last=True)

    MID = BR // 2
    top, low = pl.ds(0, MID), pl.ds(MID, MID)

    def join(src, base, group):
        def step(i, carry):
            part = pl.ds(pl.multiple_of(i * 64, 64), 64)
            here = pl.ds(pl.multiple_of(base + i * 64, 64), 64)
            src[0, part, :] = (
                src[0, part, :].astype(F32) + terms[here, rows_of(group)].astype(F32)
            ).astype(BF16)
            return carry

        lax.fori_loop(0, MID // 64, step, 0)

    def join_both():
        arrived(fl.at[0], pr.at[0, 0])
        arrived(fr.at[0], pr.at[1, 0])
        join(fl, 0, qr)
        join(fr, MID, ql)
        send(fl.at[0], fl.at[1], ps.at[0, 2], pr.at[0, 2], r, right)
        send(fr.at[0], fr.at[1], ps.at[1, 2], pr.at[1, 2], r, left)

    inverse = 1.0 / (jnp.sqrt(jnp.sum(sq[...])) + 1e-07)

    def scaled(rows):
        x_ref[rows, :] = (newm_ref[rows, :] * inverse).astype(BF16)

    tiles(scaled, 64)

    def start_sums():
        arrived(wcat.at[:, half_of(o)], wr.at[0])
        terms_half(o, q2, False)
        terms_half(o, qr, False)
        send(terms.at[top, rows_of(q2)], fl.at[0], ps.at[0, 0], pr.at[0, 0], r, right)
        send(terms.at[low, rows_of(q2)], fr.at[0], ps.at[1, 0], pr.at[1, 0], r, left)
        terms_half(o, ql, False)
        send(terms.at[low, rows_of(qr)], fl.at[2], ps.at[0, 1], pr.at[0, 1], r, right)
        terms_half(o, q0, False)
        send(terms.at[top, rows_of(ql)], fr.at[2], ps.at[1, 1], pr.at[1, 1], r, left)

    def send_update(t):
        rows = chunk(t)
        slot = ub.at[2 * r + h, rows, :]
        send(x_ref.at[rows, half_of(o)], slot, us.at[0, t], ur.at[0, t], r, c ^ 1)
        send(x_ref.at[rows, half_of(h)], slot, us.at[1, t], ur.at[1, t], r ^ 2, c)
        send(x_ref.at[rows, half_of(h)], slot, vs.at[3, t], vr.at[3, t], r ^ 1, c)

    def update_rows(rs, hs, t, own=False):
        at = 2 * rs + hs

        def step(i, carry):
            part = pl.ds(pl.multiple_of(t * CR + i * 64, 64), 64)
            here = pl.ds(pl.multiple_of(at * BR + t * CR + i * 64, 64), 64)
            new = x_ref[part, half_of(h)] if own else ub[at, part, :]
            neww_ref[here, :] = (neww_ref[here, :].astype(F32) - 8.0 * new.astype(F32)).astype(BF16)
            return carry

        lax.fori_loop(0, CR // 64, step, 0)

    load_w.wait()
    src, dst = x_ref, xb
    for step in range(NS_STEPS):
        def gram(rows):
            ab[0, rows, :] = lax.dot_general(src[rows, :], src[...], nt, preferred_element_type=F32).astype(BF16)

        def poly(rows):
            a = ab[0, rows, :]
            aa = jnp.dot(a, ab[0], preferred_element_type=F32)
            ab[1, rows, :] = (COEF_B * a.astype(F32) + COEF_C * aa).astype(BF16)

        def apply(rows):
            bx = jnp.dot(ab[1, rows, :], src[...], preferred_element_type=F32)
            dst[rows, :] = (COEF_A * src[rows, :].astype(F32) + bx).astype(BF16)

        tiles(gram)
        tiles(poly)
        if step == 0:
            start_sums()
            tiles(apply)
        else:
            apply(chunk(0))
            apply(chunk(1))
            send_update(0)
            apply(chunk(2))
            send_update(1)
            update_rows(r, h, 0, own=True)
            send_update(2)
        src, dst = dst, src

    update_rows(r, h, 1, own=True)
    update_rows(r, h, 2, own=True)
    join_both()

    def total(i, carry):
        part = pl.ds(pl.multiple_of(i * 64, 64), 64)
        below = pl.ds(pl.multiple_of(MID + i * 64, 64), 64)
        sb[part, :] = (
            terms[part, rows_of(q0)].astype(F32) + fl[1, part, :].astype(F32) + fr[2, part, :].astype(F32)
        ).astype(BF16)
        sb[below, :] = (
            terms[below, rows_of(q0)].astype(F32) + fr[1, part, :].astype(F32) + fl[2, part, :].astype(F32)
        ).astype(BF16)
        return carry

    def sum_rows(at):
        return sb.at[pl.ds(pl.multiple_of((at % 4) * FEAT, FEAT), FEAT), :]

    def pair_send():
        for k in range(2):
            send(sum_rows(2 * yb + 2 + k), sp.at[k], s2s.at[2 + k], s2r.at[2 + k], r, c ^ 2)

    def pair_sum(k):
        arrived(sp.at[k], s2r.at[2 + k])

        def add(i, carry):
            part = pl.ds(pl.multiple_of(i * 64, 64), 64)
            here = pl.ds(pl.multiple_of((2 * yb + k) * FEAT + i * 64, 64), 64)
            sb[here, :] = (sb[here, :].astype(F32) + sp[k, part, :].astype(F32)).astype(BF16)
            return carry

        lax.fori_loop(0, FEAT // 64, add, 0)
        rd, cd, own = spread_sources()[k]
        return send_spread(
            [(rd, cd, own)],
            lambda _, rd, cd: (
                remote(sum_rows(2 * yb + k), ib.at[zl], s2s.at[k], s2r.at[zl], rd, cd),
                pltpu.make_async_copy(sum_rows(2 * yb + k), ib.at[zl], s2r.at[zl]),
            ),
        )

    def relay(k, t):
        ref = ub.at[2 * froms[k][0] + froms[k][1], chunk(t), :]
        arrived(ref, ur.at[k, t])
        if k == 0:
            send(ref, ref, us.at[2, t], ur.at[2, t], r ^ 2, c)
        send(ref, ref, vs.at[k, t], vr.at[k, t], r ^ 1, c)

    def core_rows(k, t):
        rs, hs = (froms[k][0] ^ 1, froms[k][1]) if k < 3 else (r ^ 1, h)
        arrived(ub.at[2 * rs + hs, chunk(t), :], vr.at[k, t])
        update_rows(rs, hs, t)

    for t in range(2):
        relay(0, t)
        relay(1, t)
        core_rows(3, t)
        update_rows(*froms[0], t)
        update_rows(*froms[1], t)

    for ref, i, j in ((fl, 0, 1), (fr, 1, 1), (fl, 0, 2), (fr, 1, 2)):
        arrived(ref.at[3 - j], pr.at[i, j])

    lax.fori_loop(0, MID // 64, total, 0)
    core_rows(3, 2)
    pair_send()
    relay(0, 2)
    relay(1, 2)
    for t in range(CH):
        core_rows(0, t)
        if t < 2:
            core_rows(1, t)
    spreads += pair_sum(0)
    update_rows(*froms[0], 2)
    update_rows(*froms[1], 2)
    relay(2, 0)
    spreads += pair_sum(1)
    core_rows(1, 2)
    update_rows(*froms[2], 0)
    core_rows(2, 0)
    relay(2, 1)
    update_rows(*froms[2], 1)
    core_rows(2, 1)
    relay(2, 2)
    update_rows(*froms[2], 2)
    for j in range(2):
        arrived(ib.at[j], s2r.at[j])
    ig_ref[...] = (ib[0].astype(F32) + ib[1].astype(F32)).astype(BF16)
    core_rows(2, 2)

    for cp, own in spreads:
        @pl.when(jnp.logical_not(own))
        def _():
            cp.wait_send()
    for cp in others:
        cp.wait_send()


def step_call(tok, cot, weight, momentum):
    hbm = pl.BlockSpec(memory_space=pltpu.HBM)
    vm = pl.BlockSpec(memory_space=pltpu.VMEM)
    dma = pltpu.SemaphoreType.DMA
    return pl.pallas_call(
        step_kernel,
        out_shape=(
            jax.ShapeDtypeStruct((BR, BC), F32),
            jax.ShapeDtypeStruct((BR, BC), BF16),
            jax.ShapeDtypeStruct((FEAT, TOK), BF16),
            jax.ShapeDtypeStruct(weight.shape, BF16),
        ),
        in_specs=[hbm, hbm, hbm, hbm],
        out_specs=(vm, vm, vm, vm),
        scratch_shapes=[
            pltpu.VMEM((FEAT, TOK), BF16),
            pltpu.VMEM((BR, 4 * TOK), BF16),
            pltpu.VMEM((4 * TOK, BC), BF16),
            pltpu.VMEM((BR, BC), BF16),
            pltpu.VMEM((BR, 4 * TOK), F32),
            pltpu.VMEM((BR, 4 * TOK), BF16),
            pltpu.VMEM((8, HALF), F32),
            pltpu.VMEM((2, BR, BR), BF16),
            pltpu.VMEM((BR, BC), BF16),
            pltpu.VMEM((3, BR // 2, TOK), BF16),
            pltpu.VMEM((3, BR // 2, TOK), BF16),
            pltpu.VMEM((BR, TOK), BF16),
            pltpu.VMEM((2, FEAT, TOK), BF16),
            pltpu.VMEM((2, FEAT, TOK), BF16),
            pltpu.VMEM((8, BR, HALF), BF16),
            dma((4,)), dma((4,)), dma((3, 4)), dma((3, 4)), dma((3,)), dma((3,)),
            dma((4,)), dma((4,)), dma((1,)), dma((1,)), dma((5,)),
            dma((2, 3)), dma((2, 3)), dma((3, CH)), dma((3, CH)), dma((4, CH)), dma((4, CH)),
            dma((4,)), dma((4,)),
        ],
        compiler_params=pltpu.CompilerParams(
            collective_id=0, has_side_effects=True, vmem_limit_bytes=40_000_000
        ),
        cost_estimate=pl.CostEstimate(flops=14_000_000_000, bytes_accessed=20_000_000, transcendentals=0),
        name="step",
    )(tok, cot, weight, momentum)


def write_kernel(newm_ref, x_ref, ig_ref, neww_ref, newm_out, upd_out, ig_out, neww_out, buf, sem):
    copies = [
        pltpu.make_async_copy(neww_ref, neww_out, sem.at[0]),
        pltpu.make_async_copy(newm_ref, newm_out, sem.at[1]),
        pltpu.make_async_copy(ig_ref, ig_out, sem.at[2]),
    ]
    for cp in copies:
        cp.start()
    for t in range(CH):
        buf[chunk(t), :] = 32.0 * x_ref[chunk(t), :].astype(F32)
        cp = pltpu.make_async_copy(buf.at[chunk(t), :], upd_out.at[chunk(t), :], sem.at[3 + t])
        cp.start()
        copies.append(cp)
    for cp in copies:
        cp.wait()


def write_call(newm, xmat, ig, neww):
    hbm = pl.BlockSpec(memory_space=pltpu.HBM)
    vm = pl.BlockSpec(memory_space=pltpu.VMEM)
    return pl.pallas_call(
        write_kernel,
        out_shape=(
            jax.ShapeDtypeStruct(newm.shape, F32),
            jax.ShapeDtypeStruct(xmat.shape, F32),
            jax.ShapeDtypeStruct(ig.shape, BF16),
            jax.ShapeDtypeStruct(neww.shape, BF16),
        ),
        in_specs=[vm, vm, vm, vm],
        out_specs=(hbm, hbm, hbm, hbm),
        scratch_shapes=[pltpu.VMEM((BR, BC), F32), pltpu.SemaphoreType.DMA((3 + CH,))],
        compiler_params=pltpu.CompilerParams(vmem_limit_bytes=20_000_000),
        cost_estimate=pl.CostEstimate(flops=1_000_000, bytes_accessed=13_000_000, transcendentals=0),
        name="write_out",
    )(newm, xmat, ig, neww)


def body(tokens, cotangent, weight, momentum):
    pin = lambda a: pltpu.with_memory_space_constraint(a, pltpu.HBM)
    results = step_call(pin(tokens.T), pin(cotangent), pin(weight), pin(momentum[0]))
    new_momentum, update, input_grad, new_weight = write_call(*results)
    return new_weight, input_grad.T, new_momentum[None], update[None]


def solution(mesh):
    in_specs = (P("rows", "cols"), P("rows", "cols"), P(None, "cols"), P(("rows", "cols"), None, None))
    out_specs = (
        P(None, "cols"),
        P("rows", "cols"),
        P(("rows", "cols"), None, None),
        P(("rows", "cols"), None, None),
    )
    return jax.shard_map(body, mesh=mesh, in_specs=in_specs, out_specs=out_specs, check_vma=False)
```

```python
import functools

import jax
import jax.numpy as jnp
from jax import lax
from jax.experimental import pallas as pl
from jax.experimental.pallas import tpu as pltpu
from jax.sharding import PartitionSpec as P

NS_STEPS = 2
TOK = 512
FEAT = 192
BR = 768
BC = 1024
HALF = 512
COEF_A = 3.4445
COEF_B = -4.775
COEF_C = 2.0315
BETA = 0.95

MESH = pl.DeviceIdType.MESH
F32 = jnp.float32
BF16 = jnp.bfloat16


def place():
    r = lax.axis_index("rows")
    c = lax.axis_index("cols")
    return r, c, c // 8, (c // 4) % 2, c % 4


def remote(src, dst, send, recv, r, c):
    return pltpu.make_async_remote_copy(
        src_ref=src,
        dst_ref=dst,
        send_sem=send,
        recv_sem=recv,
        device_id=(r, c),
        device_id_type=MESH,
    )


def flip(v):
    return (v % 2) * 2 + v // 2


def group_at(x, r):
    return flip((x + 4 - r) % 4)


def spread_targets():
    r, c, x, zl, y = place()
    base = ((x + flip(r)) % 4) * 8 + zl + 2 * (y // 2)
    return [(x, base + 4 * k, (x == r) & (base + 4 * k == c)) for k in range(2)]


def spread_sources():
    r, c, x, zl, y = place()
    group = group_at(x, r)
    base = r * 8 + (y % 2) * 4 + 2 * (y // 2)
    return [(group, base + k, (group == r) & (base + k == c)) for k in range(2)]


def x_neighbours():
    r, c, x, zl, y = place()
    low = c % 8
    return ((x + 3) % 4) * 8 + low, ((x + 1) % 4) * 8 + low


def signal_unless(flag, barrier, r, c):
    @pl.when(jnp.logical_not(flag))
    def _():
        pl.semaphore_signal(barrier, inc=1, device_id=(r, c), device_id_type=MESH)


def entry_barrier():
    r, c, x, zl, y = place()
    left, right = x_neighbours()
    barrier = pltpu.get_barrier_semaphore()
    for rd, cd in ((r, left), (r, right), (r ^ 2, c), (r, c ^ 1), (r, c ^ 2), (r ^ 1, c)):
        pl.semaphore_signal(barrier, inc=1, device_id=(rd, cd), device_id_type=MESH)
    targets, sources = spread_targets(), spread_sources()
    for rd, cd, own in targets + sources:
        signal_unless(own, barrier, rd, cd)
    own_count = sum(jnp.where(own, 1, 0) for _, _, own in targets + sources)
    pl.semaphore_wait(barrier, 10 - own_count)


def rows_of(group):
    return pl.ds(pl.multiple_of(group * TOK, TOK), TOK)


def half_of(which):
    return pl.ds(pl.multiple_of(which * HALF, HALF), HALF)


def arrived(ref, sem):
    pltpu.make_async_copy(ref, ref, sem).wait()


def tiles(step, rows=256):
    def run(i, carry):
        step(pl.ds(pl.multiple_of(i * rows, rows), rows))
        return carry

    lax.fori_loop(0, BR // rows, run, 0)


CH = 3
CR = BR // CH


def chunk(t):
    return pl.ds(t * CR, CR)


def step_kernel(
    tok_ref, cot_ref, w_ref, mom_ref, newm_ref, x_ref, ig_ref, neww_ref,
    tokv, tokg, cotg, wcat, tacc, terms, sq, ab, xb, fl, fr, sb, sp, ib, ub,
    s1s, s1r, xs, xr, cs, cr, ds_, dr, ws, wr, ls,
    ps, pr, us, ur, vs, vr, s2s, s2r,
):
    r, c, x, zl, y = place()
    h = c % 2
    o = 1 - h
    left, right = x_neighbours()
    mine = cotg.at[rows_of(r), half_of(h)]
    own_tok = pltpu.make_async_copy(tok_ref, tokv, ls.at[0])
    own_cot = pltpu.make_async_copy(cot_ref, mine, ls.at[1])
    own_w = pltpu.make_async_copy(
        w_ref.at[pl.ds(pl.multiple_of((2 * r + h) * BR, BR), BR), :], wcat.at[:, half_of(h)], ls.at[2]
    )
    load_m = pltpu.make_async_copy(mom_ref, newm_ref, ls.at[3])
    load_w = pltpu.make_async_copy(w_ref, neww_ref, ls.at[4])
    for cp in (own_tok, own_cot, own_w, load_m, load_w):
        cp.start()
    entry_barrier()
    own_tok.wait()

    def send_spread(pairs, make):
        out = []
        for k, (rd, cd, own) in enumerate(pairs):
            cp, here = make(k, rd, cd)

            @pl.when(jnp.logical_not(own))
            def _():
                cp.start()

            @pl.when(own)
            def _():
                here.start()

            out.append((cp, own))
        return out

    def spread_tokens(k, rd, cd):
        dst = tokg.at[pl.ds(pl.multiple_of(y * FEAT, FEAT), FEAT), rows_of(r)]
        got = s1r.at[y % 2]
        return remote(tokv, dst, s1s.at[k], got, rd, cd), pltpu.make_async_copy(tokv, dst, got)

    spreads = send_spread(spread_targets(), spread_tokens)

    own_cot.wait()
    others = []

    def send(src, dst, ss, rs, rd, cd):
        cp = remote(src, dst, ss, rs, rd, cd)
        cp.start()
        others.append(cp)

    send(mine, mine, cs.at[0], cr.at[0], r, c ^ 1)
    send(mine, mine, ds_.at[3], dr.at[3], r ^ 1, c)

    q0, ql, qr, q2 = (group_at((x + k) % 4, r) for k in (0, 3, 1, 2))
    yb = y // 2

    def piece(j, group):
        at = (2 * yb + j) % 4
        return tokg.at[pl.ds(pl.multiple_of(at * FEAT, FEAT), FEAT), rows_of(group)]

    def round_x(j):
        ref = piece(j, q0)
        arrived(ref, s1r.at[j])
        if j < 2:
            send(ref, ref, s1s.at[2 + j], s1r.at[2 + j], r, c ^ 2)
        send(ref, ref, xs.at[0, j], xr.at[0, j], r, left)
        send(ref, ref, xs.at[1, j], xr.at[1, j], r, right)

    round_x(0)
    round_x(1)
    send(mine, mine, cs.at[1], cr.at[1], r ^ 2, c)

    send(
        w_ref.at[pl.ds(pl.multiple_of((2 * r + o) * BR, BR), BR), :],
        wcat.at[:, half_of(h)], ws.at[0], wr.at[0], r, c ^ 1,
    )

    froms = ((r, o), (r ^ 2, h), (r ^ 2, o))

    def pass_on(k):
        ref = cotg.at[rows_of(froms[k][0]), half_of(froms[k][1])]
        arrived(ref, cr.at[k])
        if k == 0:
            send(ref, ref, cs.at[2], cr.at[2], r ^ 2, c)
        send(ref, ref, ds_.at[k], dr.at[k], r ^ 1, c)

    def round_on(j):
        came, group, to = ((1, ql, right), (0, qr, left))[j % 2]
        ref = piece(j, group)
        arrived(ref, xr.at[came, j])
        send(ref, ref, xs.at[2, j], xr.at[2, j], r, to)

    pass_on(0)
    round_on(0)
    round_on(1)
    round_x(2)
    round_x(3)
    pass_on(1)

    def from_core(k, rs, hs):
        arrived(cotg.at[rows_of(rs), half_of(hs)], dr.at[k])

    own_w.wait()
    from_core(3, r ^ 1, h)
    from_core(1, r ^ 3, h)
    nt = (((1,), (1,)), ((), ()))

    def terms_half(which, group, first):
        def tile(rows):
            part = lax.dot_general(
                wcat[rows, half_of(which)], cotg[rows_of(group), half_of(which)], nt,
                preferred_element_type=F32,
            )
            if first:
                tacc[rows, rows_of(group)] = part
            else:
                terms[rows, rows_of(group)] = (tacc[rows, rows_of(group)] + part).astype(BF16)

        tiles(tile)

    def all_first(group, carry):
        terms_half(h, group, True)
        return carry

    lax.fori_loop(0, 4, all_first, 0)
    round_on(2)
    round_on(3)

    load_m.wait()
    sq[...] = jnp.zeros_like(sq)

    def grad_step(group, which, first=False, last=False):
        def tile(rows):
            part = jnp.dot(
                tokg[rows, rows_of(group)], cotg[rows_of(group), half_of(which)], preferred_element_type=F32
            )
            old = newm_ref[rows, half_of(which)]
            new = (BETA * old if first else old) + part
            newm_ref[rows, half_of(which)] = new
            if last:
                sq[...] += jnp.sum((new * new).reshape(-1, 8, HALF), axis=0)

        tiles(tile)

    pass_on(2)
    grad_step(q0, h, first=True)
    for j in range(4):
        came, group = ((0, qr), (1, ql))[j % 2]
        arrived(piece(j, group), xr.at[came, j])
    grad_step(ql, h)
    grad_step(qr, h)
    from_core(0, r ^ 1, o)
    from_core(2, r ^ 3, o)
    grad_step(q0, o, first=True)
    grad_step(ql, o)
    grad_step(qr, o)
    for j in range(4):
        arrived(piece(j, q2), xr.at[2, j])
    grad_step(q2, h, last=True)
    grad_step(q2, o, last=True)

    MID = BR // 2
    top, low = pl.ds(0, MID), pl.ds(MID, MID)

    def join(src, base, group):
        def step(i, carry):
            part = pl.ds(pl.multiple_of(i * 64, 64), 64)
            here = pl.ds(pl.multiple_of(base + i * 64, 64), 64)
            src[0, part, :] = (
                src[0, part, :].astype(F32) + terms[here, rows_of(group)].astype(F32)
            ).astype(BF16)
            return carry

        lax.fori_loop(0, MID // 64, step, 0)

    def join_both():
        arrived(fl.at[0], pr.at[0, 0])
        arrived(fr.at[0], pr.at[1, 0])
        join(fl, 0, qr)
        join(fr, MID, ql)
        send(fl.at[0], fl.at[1], ps.at[0, 2], pr.at[0, 2], r, right)
        send(fr.at[0], fr.at[1], ps.at[1, 2], pr.at[1, 2], r, left)

    inverse = 1.0 / (jnp.sqrt(jnp.sum(sq[...])) + 1e-07)

    def scaled(rows):
        x_ref[rows, :] = (newm_ref[rows, :] * inverse).astype(BF16)

    tiles(scaled, 64)

    def start_sums():
        arrived(wcat.at[:, half_of(o)], wr.at[0])
        terms_half(o, q2, False)
        send(terms.at[top, rows_of(q2)], fl.at[0], ps.at[0, 0], pr.at[0, 0], r, right)
        send(terms.at[low, rows_of(q2)], fr.at[0], ps.at[1, 0], pr.at[1, 0], r, left)

    def other_sums():
        terms_half(o, qr, False)
        terms_half(o, ql, False)
        send(terms.at[low, rows_of(qr)], fl.at[2], ps.at[0, 1], pr.at[0, 1], r, right)
        terms_half(o, q0, False)
        send(terms.at[top, rows_of(ql)], fr.at[2], ps.at[1, 1], pr.at[1, 1], r, left)

    def send_update(t):
        rows = chunk(t)
        slot = ub.at[2 * r + h, rows, :]
        send(x_ref.at[rows, half_of(o)], slot, us.at[0, t], ur.at[0, t], r, c ^ 1)
        send(x_ref.at[rows, half_of(h)], slot, us.at[1, t], ur.at[1, t], r ^ 2, c)
        send(x_ref.at[rows, half_of(h)], slot, vs.at[3, t], vr.at[3, t], r ^ 1, c)

    def update_rows(rs, hs, t, own=False):
        at = 2 * rs + hs

        def step(i, carry):
            part = pl.ds(pl.multiple_of(t * CR + i * 64, 64), 64)
            here = pl.ds(pl.multiple_of(at * BR + t * CR + i * 64, 64), 64)
            new = x_ref[part, half_of(h)] if own else ub[at, part, :]
            neww_ref[here, :] = (neww_ref[here, :].astype(F32) - 8.0 * new.astype(F32)).astype(BF16)
            return carry

        lax.fori_loop(0, CR // 64, step, 0)

    load_w.wait()
    src, dst = x_ref, xb
    for step in range(NS_STEPS):
        def gram(rows):
            ab[0, rows, :] = lax.dot_general(src[rows, :], src[...], nt, preferred_element_type=F32).astype(BF16)

        def poly(rows):
            a = ab[0, rows, :]
            aa = jnp.dot(a, ab[0], preferred_element_type=F32)
            ab[1, rows, :] = (COEF_B * a.astype(F32) + COEF_C * aa).astype(BF16)

        def apply(rows):
            bx = jnp.dot(ab[1, rows, :], src[...], preferred_element_type=F32)
            dst[rows, :] = (COEF_A * src[rows, :].astype(F32) + bx).astype(BF16)

        tiles(gram)
        tiles(poly)
        if step == 0:
            start_sums()
            tiles(apply)
        else:
            apply(chunk(0))
            apply(chunk(1))
            send_update(0)
            apply(chunk(2))
            send_update(1)
            update_rows(r, h, 0, own=True)
            send_update(2)
        src, dst = dst, src

    other_sums()
    update_rows(r, h, 1, own=True)
    update_rows(r, h, 2, own=True)
    join_both()

    def total(i, carry):
        part = pl.ds(pl.multiple_of(i * 64, 64), 64)
        below = pl.ds(pl.multiple_of(MID + i * 64, 64), 64)
        sb[part, :] = (
            terms[part, rows_of(q0)].astype(F32) + fl[1, part, :].astype(F32) + fr[2, part, :].astype(F32)
        ).astype(BF16)
        sb[below, :] = (
            terms[below, rows_of(q0)].astype(F32) + fr[1, part, :].astype(F32) + fl[2, part, :].astype(F32)
        ).astype(BF16)
        return carry

    def sum_rows(at):
        return sb.at[pl.ds(pl.multiple_of((at % 4) * FEAT, FEAT), FEAT), :]

    def pair_send():
        for k in range(2):
            send(sum_rows(2 * yb + 2 + k), sp.at[k], s2s.at[2 + k], s2r.at[2 + k], r, c ^ 2)

    def pair_sum(k):
        arrived(sp.at[k], s2r.at[2 + k])

        def add(i, carry):
            part = pl.ds(pl.multiple_of(i * 64, 64), 64)
            here = pl.ds(pl.multiple_of((2 * yb + k) * FEAT + i * 64, 64), 64)
            sb[here, :] = (sb[here, :].astype(F32) + sp[k, part, :].astype(F32)).astype(BF16)
            return carry

        lax.fori_loop(0, FEAT // 64, add, 0)
        rd, cd, own = spread_sources()[k]
        return send_spread(
            [(rd, cd, own)],
            lambda _, rd, cd: (
                remote(sum_rows(2 * yb + k), ib.at[zl], s2s.at[k], s2r.at[zl], rd, cd),
                pltpu.make_async_copy(sum_rows(2 * yb + k), ib.at[zl], s2r.at[zl]),
            ),
        )

    def relay(k, t):
        ref = ub.at[2 * froms[k][0] + froms[k][1], chunk(t), :]
        arrived(ref, ur.at[k, t])
        if k == 0:
            send(ref, ref, us.at[2, t], ur.at[2, t], r ^ 2, c)
        send(ref, ref, vs.at[k, t], vr.at[k, t], r ^ 1, c)

    def core_rows(k, t):
        rs, hs = (froms[k][0] ^ 1, froms[k][1]) if k < 3 else (r ^ 1, h)
        arrived(ub.at[2 * rs + hs, chunk(t), :], vr.at[k, t])
        update_rows(rs, hs, t)

    for t in range(2):
        relay(0, t)
        relay(1, t)
        core_rows(3, t)
        update_rows(*froms[0], t)
        update_rows(*froms[1], t)

    for ref, i, j in ((fl, 0, 1), (fr, 1, 1), (fl, 0, 2), (fr, 1, 2)):
        arrived(ref.at[3 - j], pr.at[i, j])

    lax.fori_loop(0, MID // 64, total, 0)
    core_rows(3, 2)
    pair_send()
    relay(0, 2)
    relay(1, 2)
    for t in range(CH):
        core_rows(0, t)
        if t < 2:
            core_rows(1, t)
    spreads += pair_sum(0)
    update_rows(*froms[0], 2)
    update_rows(*froms[1], 2)
    relay(2, 0)
    spreads += pair_sum(1)
    core_rows(1, 2)
    update_rows(*froms[2], 0)
    core_rows(2, 0)
    relay(2, 1)
    update_rows(*froms[2], 1)
    core_rows(2, 1)
    relay(2, 2)
    update_rows(*froms[2], 2)
    for j in range(2):
        arrived(ib.at[j], s2r.at[j])
    ig_ref[...] = (ib[0].astype(F32) + ib[1].astype(F32)).astype(BF16)
    core_rows(2, 2)

    for cp, own in spreads:
        @pl.when(jnp.logical_not(own))
        def _():
            cp.wait_send()
    for cp in others:
        cp.wait_send()


def step_call(tok, cot, weight, momentum):
    hbm = pl.BlockSpec(memory_space=pltpu.HBM)
    vm = pl.BlockSpec(memory_space=pltpu.VMEM)
    dma = pltpu.SemaphoreType.DMA
    return pl.pallas_call(
        step_kernel,
        out_shape=(
            jax.ShapeDtypeStruct((BR, BC), F32),
            jax.ShapeDtypeStruct((BR, BC), BF16),
            jax.ShapeDtypeStruct((FEAT, TOK), BF16),
            jax.ShapeDtypeStruct(weight.shape, BF16),
        ),
        in_specs=[hbm, hbm, hbm, hbm],
        out_specs=(vm, vm, vm, vm),
        scratch_shapes=[
            pltpu.VMEM((FEAT, TOK), BF16),
            pltpu.VMEM((BR, 4 * TOK), BF16),
            pltpu.VMEM((4 * TOK, BC), BF16),
            pltpu.VMEM((BR, BC), BF16),
            pltpu.VMEM((BR, 4 * TOK), F32),
            pltpu.VMEM((BR, 4 * TOK), BF16),
            pltpu.VMEM((8, HALF), F32),
            pltpu.VMEM((2, BR, BR), BF16),
            pltpu.VMEM((BR, BC), BF16),
            pltpu.VMEM((3, BR // 2, TOK), BF16),
            pltpu.VMEM((3, BR // 2, TOK), BF16),
            pltpu.VMEM((BR, TOK), BF16),
            pltpu.VMEM((2, FEAT, TOK), BF16),
            pltpu.VMEM((2, FEAT, TOK), BF16),
            pltpu.VMEM((8, BR, HALF), BF16),
            dma((4,)), dma((4,)), dma((3, 4)), dma((3, 4)), dma((3,)), dma((3,)),
            dma((4,)), dma((4,)), dma((1,)), dma((1,)), dma((5,)),
            dma((2, 3)), dma((2, 3)), dma((3, CH)), dma((3, CH)), dma((4, CH)), dma((4, CH)),
            dma((4,)), dma((4,)),
        ],
        compiler_params=pltpu.CompilerParams(
            collective_id=0, has_side_effects=True, vmem_limit_bytes=40_000_000
        ),
        cost_estimate=pl.CostEstimate(flops=14_000_000_000, bytes_accessed=20_000_000, transcendentals=0),
        name="step",
    )(tok, cot, weight, momentum)


def write_kernel(newm_ref, x_ref, ig_ref, neww_ref, newm_out, upd_out, ig_out, neww_out, buf, sem):
    copies = [
        pltpu.make_async_copy(neww_ref, neww_out, sem.at[0]),
        pltpu.make_async_copy(newm_ref, newm_out, sem.at[1]),
        pltpu.make_async_copy(ig_ref, ig_out, sem.at[2]),
    ]
    for cp in copies:
        cp.start()
    for t in range(CH):
        buf[chunk(t), :] = 32.0 * x_ref[chunk(t), :].astype(F32)
        cp = pltpu.make_async_copy(buf.at[chunk(t), :], upd_out.at[chunk(t), :], sem.at[3 + t])
        cp.start()
        copies.append(cp)
    for cp in copies:
        cp.wait()


def write_call(newm, xmat, ig, neww):
    hbm = pl.BlockSpec(memory_space=pltpu.HBM)
    vm = pl.BlockSpec(memory_space=pltpu.VMEM)
    return pl.pallas_call(
        write_kernel,
        out_shape=(
            jax.ShapeDtypeStruct(newm.shape, F32),
            jax.ShapeDtypeStruct(xmat.shape, F32),
            jax.ShapeDtypeStruct(ig.shape, BF16),
            jax.ShapeDtypeStruct(neww.shape, BF16),
        ),
        in_specs=[vm, vm, vm, vm],
        out_specs=(hbm, hbm, hbm, hbm),
        scratch_shapes=[pltpu.VMEM((BR, BC), F32), pltpu.SemaphoreType.DMA((3 + CH,))],
        compiler_params=pltpu.CompilerParams(vmem_limit_bytes=20_000_000),
        cost_estimate=pl.CostEstimate(flops=1_000_000, bytes_accessed=13_000_000, transcendentals=0),
        name="write_out",
    )(newm, xmat, ig, neww)


def body(tokens, cotangent, weight, momentum):
    pin = lambda a: pltpu.with_memory_space_constraint(a, pltpu.HBM)
    results = step_call(pin(tokens.T), pin(cotangent), pin(weight), pin(momentum[0]))
    new_momentum, update, input_grad, new_weight = write_call(*results)
    return new_weight, input_grad.T, new_momentum[None], update[None]


def solution(mesh):
    in_specs = (P("rows", "cols"), P("rows", "cols"), P(None, "cols"), P(("rows", "cols"), None, None))
    out_specs = (
        P(None, "cols"),
        P("rows", "cols"),
        P(("rows", "cols"), None, None),
        P(("rows", "cols"), None, None),
    )
    return jax.shard_map(body, mesh=mesh, in_specs=in_specs, out_specs=out_specs, check_vma=False)
```
